8 devices in a mesh: dp: 1 (over z), tp: 8 (over y, x, core).
Axes of the slice: x: 2, y: 2, z: 1, core: 2. Of those that a mesh axis runs over, the one named last changes fastest.
Arguments:
- hidden: bfloat16 [512, 2048], P('dp')
- w_query: bfloat16 [2048, 2048], P(None, 'tp')
- w_key: bfloat16 [2048, 256], replicated
- w_value: bfloat16 [2048, 256], replicated
- w_out: bfloat16 [2048, 2048], P('tp')
- k_cache: bfloat16 [512, 512, 256], P(('dp', 'tp'))
- v_cache: bfloat16 [512, 512, 256], P(('dp', 'tp'))
- lengths: int32 [512], P('dp')
Outputs:
- output 1: bfloat16 [512, 2048], P('dp', 'tp')
- output 2: bfloat16 [512, 512, 256], P(('dp', 'tp'))
- output 3: bfloat16 [512, 512, 256], P(('dp', 'tp'))
All inputs are finite; a program needn't handle non-finite values.
Results may differ from the reference program's by a relative error of at most 0.0162064.
Values are sent between devices in bfloat16 or wider.
A program may use at most 1 GiB of HBM per device.

```python
import jax
import jax.numpy as jnp
from jax import lax

BATCH_ROWS = 512
EMBED_DIM = 2048
Q_HEADS = 8
HEAD_DIM = 256
SEQ_LEN = 512


def setup_inputs(seed: int = 0, part: int = 0) -> dict:
    part_key = jax.random.fold_in(jax.random.key(seed), part)
    key_hid, key_kc, key_vc, key_mean, key_len, key_top = jax.random.split(part_key, 6)
    weight_keys = jax.random.split(jax.random.key(seed + 1), 4)
    total_cols = Q_HEADS * HEAD_DIM
    hidden = jax.random.normal(key_hid, (BATCH_ROWS, EMBED_DIM), jnp.float32)
    w_query = jax.random.normal(weight_keys[0], (EMBED_DIM, total_cols), jnp.float32) * EMBED_DIM ** -0.5
    w_key = jax.random.normal(weight_keys[1], (EMBED_DIM, HEAD_DIM), jnp.float32) * (2.5 * EMBED_DIM ** -0.5)
    w_value = jax.random.normal(weight_keys[2], (EMBED_DIM, HEAD_DIM), jnp.float32) * EMBED_DIM ** -0.5
    w_out = jax.random.normal(weight_keys[3], (total_cols, EMBED_DIM), jnp.float32) * total_cols ** -0.5
    k_cache = 2.5 * jax.random.normal(key_kc, (BATCH_ROWS, SEQ_LEN, HEAD_DIM), jnp.float32)
    v_mean = 0.5 * jax.random.normal(key_mean, (BATCH_ROWS, 1, HEAD_DIM), jnp.float32)
    v_cache = v_mean + jax.random.normal(key_vc, (BATCH_ROWS, SEQ_LEN, HEAD_DIM), jnp.float32)
    drawn_len = jax.random.randint(key_len, (BATCH_ROWS,), 0, SEQ_LEN)
    top_row = jax.random.randint(key_top, (), 0, BATCH_ROWS)
    lengths = jnp.where(jnp.arange(BATCH_ROWS) == top_row, SEQ_LEN - 1, drawn_len).astype(jnp.int32)
    return {
        'hidden': hidden.astype(jnp.bfloat16),
        'w_query': w_query.astype(jnp.bfloat16),
        'w_key': w_key.astype(jnp.bfloat16),
        'w_value': w_value.astype(jnp.bfloat16),
        'w_out': w_out.astype(jnp.bfloat16),
        'k_cache': k_cache.astype(jnp.bfloat16),
        'v_cache': v_cache.astype(jnp.bfloat16),
        'lengths': lengths,
    }


def rope_angles(positions):
    half_dim = HEAD_DIM // 2
    inv_freq = 10000.0 ** (-(jnp.arange(half_dim, dtype=jnp.float32) * 2.0) / HEAD_DIM)
    return positions.astype(jnp.float32)[:, None] * inv_freq[None, :]


def apply_rope(values_in, angles):
    half_dim = values_in.shape[-1] // 2
    first_half = values_in[..., :half_dim]
    second_half = values_in[..., half_dim:]
    cosines = jnp.cos(angles)
    sines = jnp.sin(angles)
    return jnp.concatenate([first_half * cosines - second_half * sines, second_half * cosines + first_half * sines], axis=-1)


def attend_row(row_args):
    q_row, k_row, v_row, length = row_args
    scores = jnp.dot(q_row, k_row.T, preferred_element_type=jnp.float32) * (HEAD_DIM ** -0.5)
    valid_mask = jnp.arange(SEQ_LEN)[None, :] <= length
    scores = jnp.where(valid_mask, scores, -1e30)
    row_max = jnp.max(scores, axis=-1, keepdims=True)
    weights = jnp.exp(scores - row_max)
    denominator = jnp.sum(weights, axis=-1, keepdims=True)
    summed = jnp.dot(weights.astype(jnp.bfloat16), v_row, preferred_element_type=jnp.float32)
    return (summed / denominator).astype(jnp.bfloat16)


def reference(hidden, w_query, w_key, w_value, w_out, k_cache, v_cache, lengths):
    q_flat = jnp.dot(hidden, w_query, preferred_element_type=jnp.float32).astype(jnp.bfloat16)
    k_new = jnp.dot(hidden, w_key, preferred_element_type=jnp.float32).astype(jnp.bfloat16)
    v_new = jnp.dot(hidden, w_value, preferred_element_type=jnp.float32).astype(jnp.bfloat16)
    angles = rope_angles(lengths)
    q_heads = q_flat.reshape(BATCH_ROWS, Q_HEADS, HEAD_DIM).astype(jnp.float32)
    q_rot = apply_rope(q_heads, angles[:, None, :]).astype(jnp.bfloat16)
    k_rot = apply_rope(k_new.astype(jnp.float32), angles).astype(jnp.bfloat16)
    new_slot = (jnp.arange(SEQ_LEN)[None, :] == lengths[:, None])[:, :, None]
    k_cache_out = jnp.where(new_slot, k_rot[:, None, :], k_cache)
    v_cache_out = jnp.where(new_slot, v_new[:, None, :], v_cache)
    attn_out = lax.map(attend_row, (q_rot, k_cache_out, v_cache_out, lengths))
    y_out = jnp.dot(attn_out.reshape(BATCH_ROWS, Q_HEADS * HEAD_DIM), w_out, preferred_element_type=jnp.float32).astype(jnp.bfloat16)
    return (y_out, k_cache_out, v_cache_out)
```

```python
import jax
import jax.numpy as jnp
from jax import lax
from jax.sharding import PartitionSpec as P


def rope_angles(positions, head_dim):
    half_dim = head_dim // 2
    inv_freq = 10000.0 ** (-(jnp.arange(half_dim, dtype=jnp.float32) * 2.0) / head_dim)
    return positions.astype(jnp.float32)[:, None] * inv_freq[None, :]


def apply_rope(values_in, angles):
    half_dim = values_in.shape[-1] // 2
    first_half = values_in[..., :half_dim]
    second_half = values_in[..., half_dim:]
    cosines = jnp.cos(angles)
    sines = jnp.sin(angles)
    return jnp.concatenate([first_half * cosines - second_half * sines, second_half * cosines + first_half * sines], axis=-1)


def attend(q_rot, k_all, v_all, lengths):
    head_dim = q_rot.shape[-1]
    seq_len = k_all.shape[1]
    scores = jnp.einsum('bhd,bsd->bhs', q_rot, k_all, preferred_element_type=jnp.float32) * (head_dim ** -0.5)
    valid_mask = lax.broadcasted_iota(jnp.int32, (1, 1, seq_len), 2) <= lengths[:, None, None]
    scores = jnp.where(valid_mask, scores, -1e30)
    row_max = jnp.max(scores, axis=-1, keepdims=True)
    weights = jnp.exp(scores - row_max)
    denominator = jnp.sum(weights, axis=-1, keepdims=True)
    summed = jnp.einsum('bhs,bsd->bhd', weights.astype(jnp.bfloat16), v_all, preferred_element_type=jnp.float32)
    return (summed / denominator).astype(jnp.bfloat16)


def solution(mesh):
    group_size = mesh.shape['tp']
    cache_spec = P(('dp', 'tp'), None, None)

    def local_step(hidden, w_query, w_key, w_value, w_out, k_cache, v_cache, lengths):
        rows_dev, seq_len, head_dim = k_cache.shape
        cols_dev = w_query.shape[1]
        num_heads = cols_dev * group_size // head_dim
        me = lax.axis_index('tp')
        row_start = me * rows_dev

        def swap(value, mask):
            return lax.ppermute(value, 'tp', [(i, i ^ mask) for i in range(group_size)])

        blocks = w_out.reshape(cols_dev, group_size, cols_dev).transpose(1, 0, 2)
        w_cols = jnp.zeros((group_size, cols_dev, cols_dev), w_out.dtype)
        for mask in range(group_size):
            block = lax.dynamic_index_in_dim(blocks, me ^ mask, 0, keepdims=True)
            w_cols = lax.dynamic_update_slice(w_cols, swap(block, mask) if mask else block, (me ^ mask, 0, 0))
        w_cols = w_cols.reshape(group_size * cols_dev, cols_dev)
        q_cols = jnp.dot(hidden, w_query, preferred_element_type=jnp.float32).astype(jnp.bfloat16)
        q_rows = lax.all_to_all(q_cols, 'tp', 0, 1, tiled=True)
        own_hidden = lax.dynamic_slice_in_dim(hidden, row_start, rows_dev, axis=0)
        own_lengths = lax.dynamic_slice_in_dim(lengths, row_start, rows_dev, axis=0)
        k_new = jnp.dot(own_hidden, w_key, preferred_element_type=jnp.float32).astype(jnp.bfloat16)
        v_new = jnp.dot(own_hidden, w_value, preferred_element_type=jnp.float32).astype(jnp.bfloat16)
        angles = rope_angles(own_lengths, head_dim)
        q_heads = q_rows.reshape(rows_dev, num_heads, head_dim).astype(jnp.float32)
        q_rot = apply_rope(q_heads, angles[:, None, :]).astype(jnp.bfloat16)
        k_rot = apply_rope(k_new.astype(jnp.float32), angles).astype(jnp.bfloat16)
        new_slot = (lax.broadcasted_iota(jnp.int32, (1, seq_len), 1) == own_lengths[:, None])[:, :, None]
        k_out = jnp.where(new_slot, k_rot[:, None, :], k_cache)
        v_out = jnp.where(new_slot, v_new[:, None, :], v_cache)
        attn_out = attend(q_rot, k_out, v_out, own_lengths)
        o_own = attn_out.reshape(rows_dev, num_heads * head_dim)
        chips = [o_own] + [swap(o_own, mask) for mask in (2, 4, 6)]
        half = jnp.stack(chips)
        sibling = swap(half, 1)
        o_all = jnp.concatenate([half, sibling]).reshape(group_size * rows_dev, num_heads * head_dim)
        y_mask = jnp.dot(o_all, w_cols, preferred_element_type=jnp.float32).astype(jnp.bfloat16)
        y_local = jnp.zeros((group_size * rows_dev, cols_dev), jnp.bfloat16)
        for slot, mask in enumerate((0, 2, 4, 6, 1, 3, 5, 7)):
            y_local = lax.dynamic_update_slice(y_local, y_mask[slot * rows_dev:(slot + 1) * rows_dev], ((me ^ mask) * rows_dev, 0))
        return y_local, k_out, v_out

    return jax.shard_map(
        local_step,
        mesh=mesh,
        in_specs=(P('dp', None), P(None, 'tp'), P(), P(), P('tp', None), cache_spec, cache_spec, P('dp')),
        out_specs=(P('dp', 'tp'), cache_spec, cache_spec),
        check_vma=False,
    )
```

```python
import functools

import jax
import jax.numpy as jnp
import numpy as np
from jax import lax
from jax.experimental import pallas as pl
from jax.experimental.pallas import tpu as pltpu
from jax.sharding import PartitionSpec as P

F32, BF16 = jnp.float32, jnp.bfloat16
HBM = pl.BlockSpec(memory_space=pltpu.HBM)
VMEM = pl.BlockSpec(memory_space=pltpu.VMEM)
SMEM = pl.BlockSpec(memory_space=pltpu.SMEM)
LOAD_ROWS = 8
CHUNKS = 2
PATCH = 16
LANES = 128


def mm(a, b):
    return jnp.dot(a, b, preferred_element_type=F32)


def rope(x, cosines, sines):
    half = x.shape[-1] // 2
    x1, x2 = x[:, :half], x[:, half:]
    return jnp.concatenate([x1 * cosines - x2 * sines, x2 * cosines + x1 * sines], axis=-1)


def step_kernel(group, lens_s, lens_v, freq, hid_h, wq_h, wk_h, wv_h, wo_h, k_h, v_h,
                k_o, v_o, kn_o, vn_o, y_o,
                hid, wq, wk, wv, wo, cosr, sinr, qrot, qbuf, qf, of, ob, obuf, wsib, psend, ybuf,
                h_sem, k_sem, v_sem, q_s, q_r, w_s, w_r, o_s, o_r, y_s, y_r):
    rows, seq, dim = k_o.shape
    batch = hid.shape[0]
    heads = group
    me = lax.axis_index('tp')
    chip, core = lax.div(me, 2), lax.rem(me, 2)
    start = me * rows
    own = pl.ds(start, rows)
    crows = rows // CHUNKS
    hrows = crows // 2
    scale = dim ** -0.5

    def remote(src, dst, ss, rs, peer):
        return pltpu.make_async_remote_copy(src_ref=src, dst_ref=dst, send_sem=ss, recv_sem=rs,
                                            device_id={'tp': peer}, device_id_type=pl.DeviceIdType.MESH)

    def other(d):
        return lax.rem(me + d, group)

    def load(src, dst, sem, i):
        part = pl.ds(i * LOAD_ROWS, LOAD_ROWS)
        return pltpu.make_async_copy(src.at[part], dst.at[part], sem.at[i])

    barrier = pltpu.get_barrier_semaphore()
    for d in range(1, group):
        pl.semaphore_signal(barrier, inc=1, device_id={'tp': other(d)}, device_id_type=pl.DeviceIdType.MESH)
    weights = [pltpu.make_async_copy(s, d, h_sem.at[i]) for i, (s, d) in enumerate(
        ((hid_h, hid), (wq_h, wq), (wk_h, wk), (wv_h, wv), (wo_h, wo)))]
    for copy in weights:
        copy.start()
    for i in range(rows // LOAD_ROWS):
        load(k_h, k_o, k_sem, i).start()
        load(v_h, v_o, v_sem, i).start()
    pos = jnp.broadcast_to(lens_v[...].astype(F32), (dim // 2, batch)).T
    angles = pos * freq[...]
    cosr[...] = jnp.cos(angles)
    sinr[...] = jnp.sin(angles)
    weights[0].wait()
    weights[1].wait()
    q = mm(hid[...], wq[...]).astype(BF16).astype(F32)
    qrot[...] = rope(q, cosr[...], sinr[...]).astype(BF16)
    pl.semaphore_wait(barrier, group - 1)

    sends = []
    for d in range(1, group):
        peer = other(d)
        copy = remote(qrot.at[pl.ds(peer * rows, rows)], qbuf.at[me], q_s.at[d], q_r.at[d], peer)
        copy.start()
        sends.append(copy)
    qbuf[me] = qrot[own, :]
    for i in range(2, 5):
        weights[i].wait()
    wcopy = remote(wo, wsib, w_s, w_r, chip * 2 + 1 - core)
    wcopy.start()
    mine = hid[own, :]
    k = mm(mine, wk[...]).astype(BF16).astype(F32)
    kn_o[...] = rope(k, cosr[own, :], sinr[own, :]).astype(BF16).astype(F32)
    vn_o[...] = mm(mine, wv[...]).astype(BF16).astype(F32)
    for copy in sends:
        copy.wait()
    for h in range(heads):
        for lane in range(2):
            qf[lane, pl.ds(h * rows, rows), :] = qbuf[h, :, lane * LANES:(lane + 1) * LANES].astype(F32)

    slot = lax.broadcasted_iota(jnp.int32, (heads, seq), 1)

    def attend(b):
        n = lens_s[start + b]
        q = jnp.concatenate([qf[lane, pl.ds(b, heads, stride=rows), :] for lane in range(2)], axis=-1)
        s = lax.dot_general(q.astype(BF16), k_o[b], (((1,), (1,)), ((), ())), preferred_element_type=F32) * scale
        s_new = jnp.sum(q * kn_o[pl.ds(b, 1), :], axis=-1, keepdims=True) * scale
        s = jnp.where(slot < n, s, -1e30)
        top = jnp.maximum(jnp.max(s, axis=-1, keepdims=True), s_new)
        e, e_new = jnp.exp(s - top), jnp.exp(s_new - top)
        total = jnp.sum(e, axis=-1, keepdims=True) + e_new
        new = e_new.astype(BF16).astype(F32) * vn_o[pl.ds(b, 1), :]
        return (mm(e.astype(BF16), v_o[b]) + new) / total

    ocopies, ycopies = [], []
    for ch in range(CHUNKS):
        def body(it, carry):
            step = ch * (crows // LOAD_ROWS) + it
            load(k_h, k_o, k_sem, step).wait()
            load(v_h, v_o, v_sem, step).wait()
            for u in range(LOAD_ROWS):
                b = it * LOAD_ROWS + u
                o = attend(ch * crows + b)
                for lane in range(2):
                    of[lane, pl.ds(b, heads, stride=crows), :] = o[:, lane * LANES:(lane + 1) * LANES]
            return carry

        lax.fori_loop(0, crows // LOAD_ROWS, body, 0)
        for h in range(heads):
            for half in range(2):
                part = pl.ds(h * crows + half * hrows, hrows)
                ob[ch, half, h] = jnp.concatenate([of[lane, part, :] for lane in range(2)], axis=-1).astype(BF16)
        copies = []
        for d in range(1, group):
            peer = other(d)
            pc, ph = lax.div(peer, 2), lax.rem(peer, 2)
            copy = remote(ob.at[ch, ph, pl.ds(pc * 2, 2)], obuf.at[ch, :, pl.ds(me * hrows, hrows)],
                          o_s.at[ch, d], o_r.at[ch, d], peer)
            copy.start()
            copies.append(copy)
        for p in range(2):
            obuf[ch, p, pl.ds(me * hrows, hrows), :] = ob[ch, core, chip * 2 + p]
        ocopies.append(copies)

    wcopy.wait()
    for ch in range(CHUNKS):
        for copy in ocopies[ch]:
            copy.wait()
        o_own, o_sib = obuf[ch, core], obuf[ch, 1 - core]
        copies = []
        for d in list(range(1, group)) + [0]:
            peer = other(d)
            cols = pl.ds(pl.multiple_of(peer * dim, dim), dim)
            part = (mm(o_own, wo[:, cols]) + mm(o_sib, wsib[:, cols])).astype(BF16)
            if d:
                psend[ch, d] = part
                copy = remote(psend.at[ch, d], ybuf.at[ch, core, chip], y_s.at[ch, d], y_r.at[ch, d], peer)
                copy.start()
                copies.append(copy)
            else:
                ybuf[ch, core, chip] = part
        ycopies.append(copies)
    for ch in range(CHUNKS):
        for copy in ycopies[ch]:
            copy.wait()
        for h in range(2):
            total = ybuf[ch, h, 0].astype(F32)
            for c in range(1, group // 2):
                total = total + ybuf[ch, h, c].astype(F32)
            total = total.astype(BF16)
            for s in range(group):
                y_o[pl.ds(s * rows + ch * crows + h * hrows, hrows), :] = total[s * hrows:(s + 1) * hrows]


def store_kernel(lens_s, k_v, v_v, kn, vn, y_i, k_o, v_o, y_o, pk, pv, k_sem, v_sem, pk_sem, pv_sem):
    rows, seq, dim = k_v.shape
    start = lax.axis_index('tp') * rows
    pairs = ((k_v, k_o, k_sem, kn, pk, pk_sem), (v_v, v_o, v_sem, vn, pv, pv_sem))

    def store(pair, i):
        part = pl.ds(i * LOAD_ROWS, LOAD_ROWS)
        return pltpu.make_async_copy(pair[0].at[part], pair[1].at[part], pair[2].at[i])

    def block(b):
        n = lens_s[start + b]
        return n, pl.multiple_of(lax.div(n, PATCH) * PATCH, PATCH)

    def patch(pair, b):
        return pltpu.make_async_copy(pair[4].at[b], pair[1].at[b, pl.ds(block(b)[1], PATCH)], pair[5].at[b])

    for i in range(rows // LOAD_ROWS):
        for pair in pairs:
            store(pair, i).start()
    y_o[...] = y_i[...]
    slot = lax.broadcasted_iota(jnp.int32, (PATCH, dim), 0)

    def fix(b, carry):
        n, base = block(b)
        for src, _, _, new, out, _ in pairs:
            old = src[b, pl.ds(base, PATCH), :].astype(F32)
            line = jnp.broadcast_to(new[pl.ds(b, 1), :], (PATCH, dim))
            out[b] = jnp.where(slot == n - base, line, old).astype(BF16)
        return carry

    lax.fori_loop(0, rows, fix, 0, unroll=4)

    def send(i, carry):
        for pair in pairs:
            store(pair, i).wait()
            for r in range(LOAD_ROWS):
                patch(pair, i * LOAD_ROWS + r).start()
        return carry

    lax.fori_loop(0, rows // LOAD_ROWS, send, 0)

    def finish(b, carry):
        for pair in pairs:
            patch(pair, b).wait()
        return carry

    lax.fori_loop(0, rows, finish, 0)


def solution(mesh):
    group = mesh.shape['tp']
    cache_spec = P(('dp', 'tp'), None, None)

    def local_step(hidden, w_query, w_key, w_value, w_out, k_cache, v_cache, lengths):
        rows, seq, dim = k_cache.shape
        batch, embed = hidden.shape
        shape = jax.ShapeDtypeStruct
        dma, mib = pltpu.SemaphoreType.DMA, 2 ** 20
        freq = np.float32(10000.0) ** (-(np.arange(dim // 2, dtype=np.float32) * np.float32(2.0)) / np.float32(dim))
        hbm = [pltpu.with_memory_space_constraint(x, pltpu.HBM)
               for x in (hidden, w_query, w_key, w_value, w_out, k_cache, v_cache)]
        steps = rows // LOAD_ROWS
        crows = rows // CHUNKS
        hrows = crows // 2
        held = pltpu.VMEM(k_cache.shape, BF16)
        k_all, v_all, k_new, v_new, y = pl.pallas_call(
            functools.partial(step_kernel, group),
            out_shape=(held, held, shape((rows, dim), F32), shape((rows, dim), F32), shape((batch, dim), BF16)),
            in_specs=[SMEM, VMEM, VMEM] + [HBM] * 7,
            out_specs=[VMEM] * 5,
            scratch_shapes=[
                pltpu.VMEM((batch, embed), BF16), pltpu.VMEM((embed, dim), BF16), pltpu.VMEM((embed, dim), BF16),
                pltpu.VMEM((embed, dim), BF16), pltpu.VMEM(w_out.shape, BF16),
                pltpu.VMEM((batch, dim // 2), F32), pltpu.VMEM((batch, dim // 2), F32), pltpu.VMEM((batch, dim), BF16),
                pltpu.VMEM((group, rows, dim), BF16), pltpu.VMEM((2, group * rows, LANES), F32),
                pltpu.VMEM((2, group * crows, LANES), F32), pltpu.VMEM((CHUNKS, 2, group, hrows, dim), BF16),
                pltpu.VMEM((CHUNKS, 2, group * hrows, dim), BF16), pltpu.VMEM(w_out.shape, BF16),
                pltpu.VMEM((CHUNKS, group, group * hrows, dim), BF16),
                pltpu.VMEM((CHUNKS, 2, group // 2, group * hrows, dim), BF16),
                dma((5,)), dma((steps,)), dma((steps,)), dma((group,)), dma((group,)), dma, dma,
                dma((CHUNKS, group)), dma((CHUNKS, group)), dma((CHUNKS, group)), dma((CHUNKS, group)),
            ],
            compiler_params=pltpu.CompilerParams(collective_id=0, has_side_effects=True, vmem_limit_bytes=14 * mib),
        )(lengths, lengths.reshape(1, batch), jnp.asarray(freq).reshape(1, dim // 2), *hbm)
        k_all, v_all = (pltpu.with_memory_space_constraint(x, pltpu.VMEM) for x in (k_all, v_all))
        k_out, v_out, y = pl.pallas_call(
            store_kernel,
            out_shape=(shape(k_cache.shape, BF16), shape(k_cache.shape, BF16), shape((batch, dim), BF16)),
            in_specs=[SMEM] + [VMEM] * 5,
            out_specs=[HBM, HBM, VMEM],
            scratch_shapes=[pltpu.VMEM((rows, PATCH, dim), BF16), pltpu.VMEM((rows, PATCH, dim), BF16),
                            dma((steps,)), dma((steps,)), dma((rows,)), dma((rows,))],
            compiler_params=pltpu.CompilerParams(vmem_limit_bytes=4 * mib),
        )(lengths, k_all, v_all, k_new, v_new, y)
        return y, k_out, v_out

    return jax.shard_map(
        local_step,
        mesh=mesh,
        in_specs=(P('dp', None), P(None, 'tp'), P(), P(), P('tp', None), cache_spec, cache_spec, P('dp')),
        out_specs=(P('dp', 'tp'), cache_spec, cache_spec),
        check_vma=False,
    )
```

```python
import functools
import math

import jax
import jax.numpy as jnp
from jax import lax
from jax.experimental import pallas as pl
from jax.experimental.pallas import tpu as pltpu
from jax.sharding import PartitionSpec as P

F32, BF16 = jnp.float32, jnp.bfloat16
HBM = pl.BlockSpec(memory_space=pltpu.HBM)
VMEM = pl.BlockSpec(memory_space=pltpu.VMEM)
LOAD_ROWS = 8
CHUNKS = 4
EARLY = 4
PATCH = 16
LANES = 128


def mm(a, b):
    return jnp.dot(a, b, preferred_element_type=F32)


def rope(x, cosines, sines):
    half = x.shape[-1] // 2
    x1, x2 = x[:, :half], x[:, half:]
    return jnp.concatenate([x1 * cosines - x2 * sines, x2 * cosines + x1 * sines], axis=-1)


def step_kernel(group, lens_h, hid_h, wq_h, wk_h, wv_h, wo_h, k_h, v_h,
                k_o, v_o, kn_o, vn_o, y_o,
                lens_s, lens_v, hid, wq, wk, wv, wo, cosr, sinr, qrot, qbuf, qf, of, ob, obuf, wsib, psend, ybuf, yf,
                h_sem, k_sem, v_sem, q_s, q_r, w_s, w_r, o_s, o_r, y_s, y_r):
    rows, seq, dim = k_o.shape
    batch = hid.shape[0]
    heads = group
    me = lax.axis_index('tp')
    chip, core = lax.div(me, 2), lax.rem(me, 2)
    start = me * rows
    own = pl.ds(start, rows)
    crows = rows // CHUNKS
    hrows = crows // 2
    scale = dim ** -0.5

    def remote(src, dst, ss, rs, peer):
        return pltpu.make_async_remote_copy(src_ref=src, dst_ref=dst, send_sem=ss, recv_sem=rs,
                                            device_id={'tp': peer}, device_id_type=pl.DeviceIdType.MESH)

    def other(d):
        return lax.rem(me + d, group)

    def load(src, dst, sem, i):
        part = pl.ds(i * LOAD_ROWS, LOAD_ROWS)
        return pltpu.make_async_copy(src.at[part], dst.at[part], sem.at[i])

    barrier = pltpu.get_barrier_semaphore()
    for d in range(1, group):
        pl.semaphore_signal(barrier, inc=1, device_id={'tp': other(d)}, device_id_type=pl.DeviceIdType.MESH)
    first = [pltpu.make_async_copy(s, d, h_sem.at[i]) for i, (s, d) in enumerate(
        ((hid_h, hid), (wq_h, wq), (lens_h, lens_v), (lens_h.at[0], lens_s)))]
    later = [pltpu.make_async_copy(s, d, h_sem.at[4 + i]) for i, (s, d) in enumerate(
        ((wk_h, wk), (wv_h, wv), (wo_h, wo)))]
    for copy in first:
        copy.start()
    first[2].wait()
    first[3].wait()
    pos = jnp.broadcast_to(lens_v[...].astype(F32), (dim // 2, batch)).T
    freq = jnp.exp(lax.broadcasted_iota(jnp.int32, (1, dim // 2), 1).astype(F32) * (-2.0 * math.log(10000.0) / dim))
    angles = pos * freq
    cosr[...] = jnp.cos(angles)
    sinr[...] = jnp.sin(angles)
    first[0].wait()
    first[1].wait()
    for copy in later:
        copy.start()
    for i in range(EARLY):
        load(k_h, k_o, k_sem, i).start()
        load(v_h, v_o, v_sem, i).start()
    q = mm(hid[...], wq[...]).astype(BF16).astype(F32)
    qrot[...] = rope(q, cosr[...], sinr[...]).astype(BF16)
    pl.semaphore_wait(barrier, group - 1)

    sends = []
    for d in range(1, group):
        peer = other(d)
        copy = remote(qrot.at[pl.ds(peer * rows, rows)], qbuf.at[me], q_s.at[d], q_r.at[d], peer)
        copy.start()
        sends.append(copy)
    qbuf[me] = qrot[own, :]
    for copy in later:
        copy.wait()
    wcopy = remote(wo, wsib, w_s, w_r, chip * 2 + 1 - core)
    wcopy.start()
    mine = hid[own, :]
    k = mm(mine, wk[...]).astype(BF16).astype(F32)
    kn_o[...] = rope(k, cosr[own, :], sinr[own, :]).astype(BF16).astype(F32)
    vn_o[...] = mm(mine, wv[...]).astype(BF16).astype(F32)
    for copy in sends:
        copy.wait()
    for i in range(EARLY, rows // LOAD_ROWS):
        load(k_h, k_o, k_sem, i).start()
        load(v_h, v_o, v_sem, i).start()
    for h in range(heads):
        for lane in range(2):
            qf[lane, pl.ds(h * rows, rows), :] = qbuf[h, :, lane * LANES:(lane + 1) * LANES].astype(F32)

    slot = lax.broadcasted_iota(jnp.int32, (heads, seq), 1)

    def attend(b):
        n = lens_s[start + b]
        q = jnp.concatenate([qf[lane, pl.ds(b, heads, stride=rows), :] for lane in range(2)], axis=-1)
        s = lax.dot_general(q.astype(BF16), k_o[b], (((1,), (1,)), ((), ())), preferred_element_type=F32) * scale
        s_new = jnp.sum(q * kn_o[pl.ds(b, 1), :], axis=-1, keepdims=True) * scale
        s = jnp.where(slot < n, s, -1e30)
        top = jnp.maximum(jnp.max(s, axis=-1, keepdims=True), s_new)
        e, e_new = jnp.exp(s - top), jnp.exp(s_new - top)
        total = jnp.sum(e, axis=-1, keepdims=True) + e_new
        new = e_new.astype(BF16).astype(F32) * vn_o[pl.ds(b, 1), :]
        return (mm(e.astype(BF16), v_o[b]) + new) / total

    ocopies, ycopies = [], []

    def attend_chunk(ch):
        def body(it, carry):
            step = ch * (crows // LOAD_ROWS) + it
            load(k_h, k_o, k_sem, step).wait()
            load(v_h, v_o, v_sem, step).wait()
            for u in range(LOAD_ROWS):
                b = it * LOAD_ROWS + u
                o = attend(ch * crows + b)
                for lane in range(2):
                    of[lane, pl.ds(b, heads, stride=crows), :] = o[:, lane * LANES:(lane + 1) * LANES]
            return carry

        lax.fori_loop(0, crows // LOAD_ROWS, body, 0)
        for h in range(heads):
            for half in range(2):
                part = pl.ds(h * crows + half * hrows, hrows)
                ob[ch, half, h] = jnp.concatenate([of[lane, part, :] for lane in range(2)], axis=-1).astype(BF16)
        copies = []
        for d in range(1, group):
            peer = other(d)
            pc, ph = lax.div(peer, 2), lax.rem(peer, 2)
            copy = remote(ob.at[ch, ph, pl.ds(pc * 2, 2)], obuf.at[ch, :, me], o_s.at[ch, d], o_r.at[ch, d], peer)
            copy.start()
            copies.append(copy)
        for p in range(2):
            obuf[ch, p, me] = ob[ch, core, chip * 2 + p]
        ocopies.append(copies)

    def project_chunk(ch):
        for copy in ocopies[ch]:
            copy.wait()
        o_own, o_sib = (obuf[ch, p].astype(F32).reshape(heads * hrows, dim).astype(BF16) for p in (core, 1 - core))
        copies = []
        for d in list(range(1, group)) + [0]:
            peer = other(d)
            cols = pl.ds(pl.multiple_of(peer * dim, dim), dim)
            part = (mm(o_own, wo[:, cols]) + mm(o_sib, wsib[:, cols])).astype(BF16)
            if d:
                psend[ch, d] = part
                copy = remote(psend.at[ch, d], ybuf.at[ch, core, chip], y_s.at[ch, d], y_r.at[ch, d], peer)
                copy.start()
                copies.append(copy)
            else:
                ybuf[ch, core, chip] = part
        ycopies.append(copies)

    def sum_chunk(ch):
        for copy in ycopies[ch]:
            copy.wait()
        for h in range(2):
            total = ybuf[ch, h, 0].astype(F32)
            for c in range(1, group // 2):
                total = total + ybuf[ch, h, c].astype(F32)
            for s in range(group):
                yf[pl.ds(s * rows + ch * crows + h * hrows, hrows), :] = total[s * hrows:(s + 1) * hrows]

    for ch in range(CHUNKS):
        attend_chunk(ch)
        if ch == 0:
            wcopy.wait()
        else:
            project_chunk(ch - 1)
    project_chunk(CHUNKS - 1)
    for ch in range(CHUNKS):
        sum_chunk(ch)
    y_o[...] = yf[...].astype(BF16)


def store_kernel(lens_h, k_i, v_i, kn, vn, y_i, k_o, v_o, y_o, k_v, v_v, lens_s, l_sem, k_sem, v_sem):
    rows, seq, dim = k_v.shape
    start = lax.axis_index('tp') * rows
    pairs = ((k_v, k_o, k_sem, kn), (v_v, v_o, v_sem, vn))

    def store(pair, i):
        part = pl.ds(i * LOAD_ROWS, LOAD_ROWS)
        return pltpu.make_async_copy(pair[0].at[part], pair[1].at[part], pair[2].at[i])

    lens = pltpu.make_async_copy(lens_h.at[0], lens_s, l_sem)
    lens.start()
    y_o[...] = y_i[...]
    slot = lax.broadcasted_iota(jnp.int32, (PATCH, dim), 0)
    lens.wait()

    def send(i, carry):
        for pair in pairs:
            ref, new = pair[0], pair[3]
            for r in range(LOAD_ROWS):
                b = i * LOAD_ROWS + r
                n = lens_s[start + b]
                base = pl.multiple_of(lax.div(n, PATCH) * PATCH, PATCH)
                line = jnp.broadcast_to(new[pl.ds(b, 1), :], (PATCH, dim))
                old = ref[b, pl.ds(base, PATCH), :].astype(F32)
                ref[b, pl.ds(base, PATCH), :] = jnp.where(slot == n - base, line, old).astype(BF16)
            store(pair, i).start()
        return carry

    lax.fori_loop(0, rows // LOAD_ROWS, send, 0)
    for i in range(rows // LOAD_ROWS):
        for pair in pairs:
            store(pair, i).wait()


def solution(mesh):
    group = mesh.shape['tp']
    cache_spec = P(('dp', 'tp'), None, None)

    def local_step(hidden, w_query, w_key, w_value, w_out, k_cache, v_cache, lengths):
        rows, seq, dim = k_cache.shape
        batch, embed = hidden.shape
        shape = jax.ShapeDtypeStruct
        dma, mib = pltpu.SemaphoreType.DMA, 2 ** 20
        hbm = [pltpu.with_memory_space_constraint(x, pltpu.HBM)
               for x in (lengths.reshape(1, batch), hidden, w_query, w_key, w_value, w_out, k_cache, v_cache)]
        steps = rows // LOAD_ROWS
        crows = rows // CHUNKS
        hrows = crows // 2
        held = pltpu.VMEM(k_cache.shape, BF16)
        k_all, v_all, k_new, v_new, y = pl.pallas_call(
            functools.partial(step_kernel, group),
            out_shape=(held, held, shape((rows, dim), F32), shape((rows, dim), F32), shape((batch, dim), BF16)),
            in_specs=[HBM] * 8,
            out_specs=[VMEM] * 5,
            scratch_shapes=[
                pltpu.SMEM((batch,), jnp.int32), pltpu.VMEM((1, batch), jnp.int32),
                pltpu.VMEM((batch, embed), BF16), pltpu.VMEM((embed, dim), BF16), pltpu.VMEM((embed, dim), BF16),
                pltpu.VMEM((embed, dim), BF16), pltpu.VMEM(w_out.shape, BF16),
                pltpu.VMEM((batch, dim // 2), F32), pltpu.VMEM((batch, dim // 2), F32), pltpu.VMEM((batch, dim), BF16),
                pltpu.VMEM((group, rows, dim), BF16), pltpu.VMEM((2, group * rows, LANES), F32),
                pltpu.VMEM((2, group * crows, LANES), F32), pltpu.VMEM((CHUNKS, 2, group, hrows, dim), BF16),
                pltpu.VMEM((CHUNKS, 2, group, hrows, dim), BF16), pltpu.VMEM(w_out.shape, BF16),
                pltpu.VMEM((CHUNKS, group, group * hrows, dim), BF16),
                pltpu.VMEM((CHUNKS, 2, group // 2, group * hrows, dim), BF16), pltpu.VMEM((batch, dim), F32),
                dma((7,)), dma((steps,)), dma((steps,)), dma((group,)), dma((group,)), dma, dma,
                dma((CHUNKS, group)), dma((CHUNKS, group)), dma((CHUNKS, group)), dma((CHUNKS, group)),
            ],
            compiler_params=pltpu.CompilerParams(collective_id=0, has_side_effects=True, vmem_limit_bytes=14 * mib),
        )(*hbm)
        k_all, v_all = (pltpu.with_memory_space_constraint(x, pltpu.VMEM) for x in (k_all, v_all))
        k_out, v_out, y, _, _ = pl.pallas_call(
            store_kernel,
            out_shape=(shape(k_cache.shape, BF16), shape(k_cache.shape, BF16), shape((batch, dim), BF16), held, held),
            in_specs=[HBM] + [VMEM] * 5,
            out_specs=[HBM, HBM, VMEM, VMEM, VMEM],
            input_output_aliases={1: 3, 2: 4},
            scratch_shapes=[pltpu.SMEM((batch,), jnp.int32), dma, dma((steps,)), dma((steps,))],
            compiler_params=pltpu.CompilerParams(vmem_limit_bytes=4 * mib),
        )(hbm[0], k_all, v_all, k_new, v_new, y)
        return y, k_out, v_out

    return jax.shard_map(
        local_step,
        mesh=mesh,
        in_specs=(P('dp', None), P(None, 'tp'), P(), P(), P('tp', None), cache_spec, cache_spec, P('dp')),
        out_specs=(P('dp', 'tp'), cache_spec, cache_spec),
        check_vma=False,
    )
```

```python
import functools
import math

import jax
import jax.numpy as jnp
from jax import lax
from jax.experimental import pallas as pl
from jax.experimental.pallas import tpu as pltpu
from jax.sharding import PartitionSpec as P

F32, BF16 = jnp.float32, jnp.bfloat16
HBM = pl.BlockSpec(memory_space=pltpu.HBM)
VMEM = pl.BlockSpec(memory_space=pltpu.VMEM)
LOAD_ROWS = 8
CHUNKS = 2
EARLY = 4
PATCH = 16
LANES = 128


def mm(a, b):
    return jnp.dot(a, b, preferred_element_type=F32)


def rope(x, cosines, sines):
    half = x.shape[-1] // 2
    x1, x2 = x[:, :half], x[:, half:]
    return jnp.concatenate([x1 * cosines - x2 * sines, x2 * cosines + x1 * sines], axis=-1)


def step_kernel(group, lens_h, hid_h, wq_h, wk_h, wv_h, wo_h, k_h, v_h,
                k_o, v_o, kn_o, vn_o, y_o,
                lens_s, lens_v, hid, wq, wk, wv, wo, cosr, sinr, qrot, qbuf, qf, of, ob, obuf, wsib, psend, ybuf, yf,
                h_sem, k_sem, v_sem, q_s, q_r, w_s, w_r, o_s, o_r, y_s, y_r):
    rows, seq, dim = k_o.shape
    batch = hid.shape[0]
    heads = group
    me = lax.axis_index('tp')
    chip, core = lax.div(me, 2), lax.rem(me, 2)
    start = me * rows
    own = pl.ds(start, rows)
    crows = rows // CHUNKS
    hrows = crows // 2
    scale = dim ** -0.5

    def remote(src, dst, ss, rs, peer):
        return pltpu.make_async_remote_copy(src_ref=src, dst_ref=dst, send_sem=ss, recv_sem=rs,
                                            device_id={'tp': peer}, device_id_type=pl.DeviceIdType.MESH)

    def other(d):
        return lax.rem(me + d, group)

    def load(src, dst, sem, i):
        part = pl.ds(i * LOAD_ROWS, LOAD_ROWS)
        return pltpu.make_async_copy(src.at[part], dst.at[part], sem.at[i])

    barrier = pltpu.get_barrier_semaphore()
    for d in range(1, group):
        pl.semaphore_signal(barrier, inc=1, device_id={'tp': other(d)}, device_id_type=pl.DeviceIdType.MESH)
    first = [pltpu.make_async_copy(s, d, h_sem.at[i]) for i, (s, d) in enumerate(
        ((hid_h, hid), (wq_h, wq), (lens_h, lens_v), (lens_h.at[0], lens_s)))]
    later = [pltpu.make_async_copy(s, d, h_sem.at[4 + i]) for i, (s, d) in enumerate(
        ((wk_h, wk), (wv_h, wv), (wo_h, wo)))]
    for copy in first + later:
        copy.start()
    first[2].wait()
    first[3].wait()
    pos = jnp.broadcast_to(lens_v[...].astype(F32), (dim // 2, batch)).T
    freq = jnp.exp(lax.broadcasted_iota(jnp.int32, (1, dim // 2), 1).astype(F32) * (-2.0 * math.log(10000.0) / dim))
    angles = pos * freq
    cosr[...] = jnp.cos(angles)
    sinr[...] = jnp.sin(angles)
    first[0].wait()
    first[1].wait()
    for i in range(EARLY):
        load(k_h, k_o, k_sem, i).start()
        load(v_h, v_o, v_sem, i).start()
    q = mm(hid[...], wq[...]).astype(BF16).astype(F32)
    qrot[...] = rope(q, cosr[...], sinr[...]).astype(BF16)
    pl.semaphore_wait(barrier, group - 1)

    sends = []
    for d in range(1, group):
        peer = other(d)
        copy = remote(qrot.at[pl.ds(peer * rows, rows)], qbuf.at[me], q_s.at[d], q_r.at[d], peer)
        copy.start()
        sends.append(copy)
    qbuf[me] = qrot[own, :]
    for copy in later:
        copy.wait()
    wcopy = remote(wo, wsib, w_s, w_r, chip * 2 + 1 - core)
    wcopy.start()
    mine = hid[own, :]
    k = mm(mine, wk[...]).astype(BF16).astype(F32)
    kn_o[...] = rope(k, cosr[own, :], sinr[own, :]).astype(BF16).astype(F32)
    vn_o[...] = mm(mine, wv[...]).astype(BF16).astype(F32)
    for copy in sends:
        copy.wait()
    for i in range(EARLY, rows // LOAD_ROWS):
        load(k_h, k_o, k_sem, i).start()
        load(v_h, v_o, v_sem, i).start()
    for h in range(heads):
        for lane in range(2):
            qf[lane, pl.ds(h * rows, rows), :] = qbuf[h, :, lane * LANES:(lane + 1) * LANES].astype(F32)

    slot = lax.broadcasted_iota(jnp.int32, (heads, seq), 1)

    def attend(b):
        n = lens_s[start + b]
        q = jnp.concatenate([qf[lane, pl.ds(b, heads, stride=rows), :] for lane in range(2)], axis=-1)
        s = lax.dot_general(q.astype(BF16), k_o[b], (((1,), (1,)), ((), ())), preferred_element_type=F32) * scale
        s_new = jnp.sum(q * kn_o[pl.ds(b, 1), :], axis=-1, keepdims=True) * scale
        s = jnp.where(slot < n, s, -1e30)
        top = jnp.maximum(jnp.max(s, axis=-1, keepdims=True), s_new)
        e, e_new = jnp.exp(s - top), jnp.exp(s_new - top)
        total = jnp.sum(e, axis=-1, keepdims=True) + e_new
        new = e_new.astype(BF16).astype(F32) * vn_o[pl.ds(b, 1), :]
        return (mm(e.astype(BF16), v_o[b]) + new) / total

    ocopies, ycopies = [], []

    def attend_chunk(ch):
        def body(it, carry):
            step = ch * (crows // LOAD_ROWS) + it
            load(k_h, k_o, k_sem, step).wait()
            load(v_h, v_o, v_sem, step).wait()
            for u in range(LOAD_ROWS):
                b = it * LOAD_ROWS + u
                o = attend(ch * crows + b)
                for lane in range(2):
                    of[lane, pl.ds(b, heads, stride=crows), :] = o[:, lane * LANES:(lane + 1) * LANES]
            return carry

        lax.fori_loop(0, crows // LOAD_ROWS, body, 0)
        for h in range(heads):
            for half in range(2):
                part = pl.ds(h * crows + half * hrows, hrows)
                ob[ch, half, h] = jnp.concatenate([of[lane, part, :] for lane in range(2)], axis=-1).astype(BF16)
        copies = []
        for d in range(1, group):
            peer = other(d)
            pc, ph = lax.div(peer, 2), lax.rem(peer, 2)
            copy = remote(ob.at[ch, ph, pl.ds(pc * 2, 2)], obuf.at[ch, :, me], o_s.at[ch, d], o_r.at[ch, d], peer)
            copy.start()
            copies.append(copy)
        for p in range(2):
            obuf[ch, p, me] = ob[ch, core, chip * 2 + p]
        ocopies.append(copies)

    def project_chunk(ch):
        for copy in ocopies[ch]:
            copy.wait()
        o_own, o_sib = (obuf[ch, p].astype(F32).reshape(heads * hrows, dim).astype(BF16) for p in (core, 1 - core))
        copies = []
        for d in list(range(1, group)) + [0]:
            peer = other(d)
            cols = pl.ds(pl.multiple_of(peer * dim, dim), dim)
            part = (mm(o_own, wo[:, cols]) + mm(o_sib, wsib[:, cols])).astype(BF16)
            if d:
                psend[ch, d] = part
                copy = remote(psend.at[ch, d], ybuf.at[ch, core, chip], y_s.at[ch, d], y_r.at[ch, d], peer)
                copy.start()
                copies.append(copy)
            else:
                ybuf[ch, core, chip] = part
        ycopies.append(copies)

    def sum_chunk(ch):
        for copy in ycopies[ch]:
            copy.wait()
        for h in range(2):
            total = ybuf[ch, h, 0].astype(F32)
            for c in range(1, group // 2):
                total = total + ybuf[ch, h, c].astype(F32)
            for s in range(group):
                yf[pl.ds(s * rows + ch * crows + h * hrows, hrows), :] = total[s * hrows:(s + 1) * hrows]

    for ch in range(CHUNKS):
        attend_chunk(ch)
        if ch == 0:
            wcopy.wait()
        else:
            project_chunk(ch - 1)
    project_chunk(CHUNKS - 1)
    for ch in range(CHUNKS):
        sum_chunk(ch)
    y_o[...] = yf[...].astype(BF16)


def store_kernel(lens_h, k_i, v_i, kn, vn, y_i, k_o, v_o, y_o, k_v, v_v, lens_s, l_sem, k_sem, v_sem):
    rows, seq, dim = k_v.shape
    start = lax.axis_index('tp') * rows
    pairs = ((k_v, k_o, k_sem, kn), (v_v, v_o, v_sem, vn))

    def store(pair, i):
        part = pl.ds(i * LOAD_ROWS, LOAD_ROWS)
        return pltpu.make_async_copy(pair[0].at[part], pair[1].at[part], pair[2].at[i])

    lens = pltpu.make_async_copy(lens_h.at[0], lens_s, l_sem)
    lens.start()
    y_o[...] = y_i[...]
    slot = lax.broadcasted_iota(jnp.int32, (PATCH, dim), 0)
    lens.wait()

    def send(i, carry):
        for pair in pairs:
            ref, new = pair[0], pair[3]
            for r in range(LOAD_ROWS):
                b = i * LOAD_ROWS + r
                n = lens_s[start + b]
                base = pl.multiple_of(lax.div(n, PATCH) * PATCH, PATCH)
                line = jnp.broadcast_to(new[pl.ds(b, 1), :], (PATCH, dim))
                old = ref[b, pl.ds(base, PATCH), :].astype(F32)
                ref[b, pl.ds(base, PATCH), :] = jnp.where(slot == n - base, line, old).astype(BF16)
            store(pair, i).start()
        return carry

    lax.fori_loop(0, rows // LOAD_ROWS, send, 0)
    for i in range(rows // LOAD_ROWS):
        for pair in pairs:
            store(pair, i).wait()


def solution(mesh):
    group = mesh.shape['tp']
    cache_spec = P(('dp', 'tp'), None, None)

    def local_step(hidden, w_query, w_key, w_value, w_out, k_cache, v_cache, lengths):
        rows, seq, dim = k_cache.shape
        batch, embed = hidden.shape
        shape = jax.ShapeDtypeStruct
        dma, mib = pltpu.SemaphoreType.DMA, 2 ** 20
        hbm = [pltpu.with_memory_space_constraint(x, pltpu.HBM)
               for x in (lengths.reshape(1, batch), hidden, w_query, w_key, w_value, w_out, k_cache, v_cache)]
        steps = rows // LOAD_ROWS
        crows = rows // CHUNKS
        hrows = crows // 2
        held = pltpu.VMEM(k_cache.shape, BF16)
        k_all, v_all, k_new, v_new, y = pl.pallas_call(
            functools.partial(step_kernel, group),
            out_shape=(held, held, shape((rows, dim), F32), shape((rows, dim), F32), shape((batch, dim), BF16)),
            in_specs=[HBM] * 8,
            out_specs=[VMEM] * 5,
            scratch_shapes=[
                pltpu.SMEM((batch,), jnp.int32), pltpu.VMEM((1, batch), jnp.int32),
                pltpu.VMEM((batch, embed), BF16), pltpu.VMEM((embed, dim), BF16), pltpu.VMEM((embed, dim), BF16),
                pltpu.VMEM((embed, dim), BF16), pltpu.VMEM(w_out.shape, BF16),
                pltpu.VMEM((batch, dim // 2), F32), pltpu.VMEM((batch, dim // 2), F32), pltpu.VMEM((batch, dim), BF16),
                pltpu.VMEM((group, rows, dim), BF16), pltpu.VMEM((2, group * rows, LANES), F32),
                pltpu.VMEM((2, group * crows, LANES), F32), pltpu.VMEM((CHUNKS, 2, group, hrows, dim), BF16),
                pltpu.VMEM((CHUNKS, 2, group, hrows, dim), BF16), pltpu.VMEM(w_out.shape, BF16),
                pltpu.VMEM((CHUNKS, group, group * hrows, dim), BF16),
                pltpu.VMEM((CHUNKS, 2, group // 2, group * hrows, dim), BF16), pltpu.VMEM((batch, dim), F32),
                dma((7,)), dma((steps,)), dma((steps,)), dma((group,)), dma((group,)), dma, dma,
                dma((CHUNKS, group)), dma((CHUNKS, group)), dma((CHUNKS, group)), dma((CHUNKS, group)),
            ],
            compiler_params=pltpu.CompilerParams(collective_id=0, has_side_effects=True, vmem_limit_bytes=14 * mib),
        )(*hbm)
        k_all, v_all = (pltpu.with_memory_space_constraint(x, pltpu.VMEM) for x in (k_all, v_all))
        k_out, v_out, y, _, _ = pl.pallas_call(
            store_kernel,
            out_shape=(shape(k_cache.shape, BF16), shape(k_cache.shape, BF16), shape((batch, dim), BF16), held, held),
            in_specs=[HBM] + [VMEM] * 5,
            out_specs=[HBM, HBM, VMEM, VMEM, VMEM],
            input_output_aliases={1: 3, 2: 4},
            scratch_shapes=[pltpu.SMEM((batch,), jnp.int32), dma, dma((steps,)), dma((steps,))],
            compiler_params=pltpu.CompilerParams(vmem_limit_bytes=4 * mib),
        )(hbm[0], k_all, v_all, k_new, v_new, y)
        return y, k_out, v_out

    return jax.shard_map(
        local_step,
        mesh=mesh,
        in_specs=(P('dp', None), P(None, 'tp'), P(), P(), P('tp', None), cache_spec, cache_spec, P('dp')),
        out_specs=(P('dp', 'tp'), cache_spec, cache_spec),
        check_vma=False,
    )
```

```python
import functools
import math

import jax
import jax.numpy as jnp
from jax import lax
from jax.experimental import pallas as pl
from jax.experimental.pallas import tpu as pltpu
from jax.sharding import PartitionSpec as P

F32, BF16 = jnp.float32, jnp.bfloat16
HBM = pl.BlockSpec(memory_space=pltpu.HBM)
VMEM = pl.BlockSpec(memory_space=pltpu.VMEM)
LOAD_ROWS = 8
CHUNKS = 4
EARLY = 4
PATCH = 16
LANES = 128
GROUP = 4


def mm(a, b):
    return jnp.dot(a, b, preferred_element_type=F32)


def rope(x, cosines, sines):
    half = x.shape[-1] // 2
    x1, x2 = x[:, :half], x[:, half:]
    return jnp.concatenate([x1 * cosines - x2 * sines, x2 * cosines + x1 * sines], axis=-1)


def step_kernel(group, lens_h, hid_h, wq_h, wk_h, wv_h, wo_h, k_h, v_h,
                k_o, v_o, kn_o, vn_o, y_o,
                lens_s, lens_v, hid, wq, wk, wv, wo, cosr, sinr, qrot, qbuf, qf, of, ob, obuf, wsib, psend, ybuf, yf,
                h_sem, k_sem, v_sem, q_s, q_r, w_s, w_r, o_s, o_r, y_s, y_r):
    rows, seq, dim = k_o.shape
    batch = hid.shape[0]
    heads = group
    me = lax.axis_index('tp')
    chip, core = lax.div(me, 2), lax.rem(me, 2)
    start = me * rows
    own = pl.ds(start, rows)
    crows = rows // CHUNKS
    hrows = crows // 2
    scale = dim ** -0.5

    def remote(src, dst, ss, rs, peer):
        return pltpu.make_async_remote_copy(src_ref=src, dst_ref=dst, send_sem=ss, recv_sem=rs,
                                            device_id={'tp': peer}, device_id_type=pl.DeviceIdType.MESH)

    def other(d):
        return lax.rem(me + d, group)

    def load(src, dst, sem, i):
        part = pl.ds(i * LOAD_ROWS, LOAD_ROWS)
        return pltpu.make_async_copy(src.at[part], dst.at[part], sem.at[i])

    barrier = pltpu.get_barrier_semaphore()
    for d in range(1, group):
        pl.semaphore_signal(barrier, inc=1, device_id={'tp': other(d)}, device_id_type=pl.DeviceIdType.MESH)
    first = [pltpu.make_async_copy(s, d, h_sem.at[i]) for i, (s, d) in enumerate(
        ((hid_h, hid), (wq_h, wq), (lens_h, lens_v), (lens_h.at[0], lens_s)))]
    later = [pltpu.make_async_copy(s, d, h_sem.at[4 + i]) for i, (s, d) in enumerate(
        ((wk_h, wk), (wv_h, wv), (wo_h, wo)))]
    for copy in first + later:
        copy.start()
    first[2].wait()
    first[3].wait()
    pos = jnp.broadcast_to(lens_v[...].astype(F32), (dim // 2, batch)).T
    freq = jnp.exp(lax.broadcasted_iota(jnp.int32, (1, dim // 2), 1).astype(F32) * (-2.0 * math.log(10000.0) / dim))
    angles = pos * freq
    cosr[...] = jnp.cos(angles)
    sinr[...] = jnp.sin(angles)
    first[0].wait()
    first[1].wait()
    for i in range(EARLY):
        load(k_h, k_o, k_sem, i).start()
        load(v_h, v_o, v_sem, i).start()
    q = mm(hid[...], wq[...]).astype(BF16).astype(F32)
    qrot[...] = rope(q, cosr[...], sinr[...]).astype(BF16)
    pl.semaphore_wait(barrier, group - 1)

    sends = []
    for d in range(1, group):
        peer = other(d)
        copy = remote(qrot.at[pl.ds(peer * rows, rows)], qbuf.at[me], q_s.at[d], q_r.at[d], peer)
        copy.start()
        sends.append(copy)
    qbuf[me] = qrot[own, :]
    for copy in later:
        copy.wait()
    wcopy = remote(wo, wsib, w_s, w_r, chip * 2 + 1 - core)
    wcopy.start()
    mine = hid[own, :]
    k = mm(mine, wk[...]).astype(BF16).astype(F32)
    kn_o[...] = rope(k, cosr[own, :], sinr[own, :]).astype(BF16).astype(F32)
    vn_o[...] = mm(mine, wv[...]).astype(BF16).astype(F32)
    for copy in sends:
        copy.wait()
    for i in range(EARLY, rows // LOAD_ROWS):
        load(k_h, k_o, k_sem, i).start()
        load(v_h, v_o, v_sem, i).start()
    for h in range(heads):
        for lane in range(2):
            qf[lane, pl.ds(h * (rows + 1), rows), :] = qbuf[h, :, lane * LANES:(lane + 1) * LANES].astype(F32)

    slot = lax.broadcasted_iota(jnp.int32, (heads, seq), 1)

    def scores(b):
        n = lens_s[start + b]
        q = jnp.concatenate([qf[lane, pl.ds(b, heads, stride=rows + 1), :] for lane in range(2)], axis=-1)
        s = lax.dot_general(q.astype(BF16), k_o[b], (((1,), (1,)), ((), ())), preferred_element_type=F32) * scale
        s_new = jnp.sum(q * kn_o[pl.ds(b, 1), :], axis=-1, keepdims=True) * scale
        return jnp.where(slot < n, s, -1e30), s_new

    def softmax(s, s_new):
        top = jnp.maximum(jnp.max(s, axis=-1, keepdims=True), s_new)
        e, e_new = jnp.exp(s - top), jnp.exp(s_new - top)
        return e.astype(BF16), e_new.astype(BF16).astype(F32), jnp.sum(e, axis=-1, keepdims=True) + e_new

    def attend(first_row, crow):
        groups = [range(g, g + GROUP) for g in range(0, crow, GROUP)]
        ready = None
        for g in range(len(groups) + 1):
            nxt = [scores(first_row + u) for u in groups[g]] if g < len(groups) else None
            if ready is not None:
                soft = [softmax(*pair) for pair in ready]
                outs = [mm(e, v_o[first_row + u]) for (e, _, _), u in zip(soft, groups[g - 1])]
                for o, (_, e_new, total), u in zip(outs, soft, groups[g - 1]):
                    o = (o + e_new * vn_o[pl.ds(first_row + u, 1), :]) / total
                    for lane in range(2):
                        of[lane, pl.ds(u, heads, stride=crow + 1), :] = o[:, lane * LANES:(lane + 1) * LANES]
            ready = nxt

    ocopies, ycopies = [], []

    def attend_chunk(ch):
        for step in range(ch * crows // LOAD_ROWS, (ch + 1) * crows // LOAD_ROWS):
            load(k_h, k_o, k_sem, step).wait()
            load(v_h, v_o, v_sem, step).wait()
        attend(ch * crows, crows)
        for h in range(heads):
            for half in range(2):
                part = pl.ds(h * (crows + 1) + half * hrows, hrows)
                ob[ch, half, h] = jnp.concatenate([of[lane, part, :] for lane in range(2)], axis=-1).astype(BF16)
        copies = []
        for d in range(1, group):
            peer = other(d)
            pc, ph = lax.div(peer, 2), lax.rem(peer, 2)
            copy = remote(ob.at[ch, ph, pl.ds(pc * 2, 2)], obuf.at[ch, :, me], o_s.at[ch, d], o_r.at[ch, d], peer)
            copy.start()
            copies.append(copy)
        for p in range(2):
            obuf[ch, p, me] = ob[ch, core, chip * 2 + p]
        ocopies.append(copies)

    def project_chunk(ch):
        for copy in ocopies[ch]:
            copy.wait()
        o_own, o_sib = (obuf[ch, p].astype(F32).reshape(heads * hrows, dim).astype(BF16) for p in (core, 1 - core))
        copies = []
        for d in list(range(1, group)) + [0]:
            peer = other(d)
            cols = pl.ds(pl.multiple_of(peer * dim, dim), dim)
            part = (mm(o_own, wo[:, cols]) + mm(o_sib, wsib[:, cols])).astype(BF16)
            if d:
                psend[ch, d] = part
                copy = remote(psend.at[ch, d], ybuf.at[ch, core, chip], y_s.at[ch, d], y_r.at[ch, d], peer)
                copy.start()
                copies.append(copy)
            else:
                ybuf[ch, core, chip] = part
        ycopies.append(copies)

    def sum_chunk(ch):
        for copy in ycopies[ch]:
            copy.wait()
        for h in range(2):
            total = ybuf[ch, h, 0].astype(F32)
            for c in range(1, group // 2):
                total = total + ybuf[ch, h, c].astype(F32)
            for s in range(group):
                yf[pl.ds(s * rows + ch * crows + h * hrows, hrows), :] = total[s * hrows:(s + 1) * hrows]

    for ch in range(CHUNKS):
        attend_chunk(ch)
        if ch == 0:
            wcopy.wait()
        else:
            project_chunk(ch - 1)
    project_chunk(CHUNKS - 1)
    for ch in range(CHUNKS):
        sum_chunk(ch)
    y_o[...] = yf[...].astype(BF16)


def store_kernel(lens_h, k_i, v_i, kn, vn, y_i, k_o, v_o, y_o, k_v, v_v, lens_s, l_sem, k_sem, v_sem):
    rows, seq, dim = k_v.shape
    start = lax.axis_index('tp') * rows
    pairs = ((k_v, k_o, k_sem, kn), (v_v, v_o, v_sem, vn))

    def store(pair, i):
        part = pl.ds(i * LOAD_ROWS, LOAD_ROWS)
        return pltpu.make_async_copy(pair[0].at[part], pair[1].at[part], pair[2].at[i])

    lens = pltpu.make_async_copy(lens_h.at[0], lens_s, l_sem)
    lens.start()
    y_o[...] = y_i[...]
    slot = lax.broadcasted_iota(jnp.int32, (PATCH, dim), 0)
    lens.wait()

    def send(i, carry):
        for pair in pairs:
            ref, new = pair[0], pair[3]
            for r in range(LOAD_ROWS):
                b = i * LOAD_ROWS + r
                n = lens_s[start + b]
                base = pl.multiple_of(lax.div(n, PATCH) * PATCH, PATCH)
                line = jnp.broadcast_to(new[pl.ds(b, 1), :], (PATCH, dim))
                old = ref[b, pl.ds(base, PATCH), :].astype(F32)
                ref[b, pl.ds(base, PATCH), :] = jnp.where(slot == n - base, line, old).astype(BF16)
            store(pair, i).start()
        return carry

    lax.fori_loop(0, rows // LOAD_ROWS, send, 0)
    for i in range(rows // LOAD_ROWS):
        for pair in pairs:
            store(pair, i).wait()


def solution(mesh):
    group = mesh.shape['tp']
    cache_spec = P(('dp', 'tp'), None, None)

    def local_step(hidden, w_query, w_key, w_value, w_out, k_cache, v_cache, lengths):
        rows, seq, dim = k_cache.shape
        batch, embed = hidden.shape
        shape = jax.ShapeDtypeStruct
        dma, mib = pltpu.SemaphoreType.DMA, 2 ** 20
        hbm = [pltpu.with_memory_space_constraint(x, pltpu.HBM)
               for x in (lengths.reshape(1, batch), hidden, w_query, w_key, w_value, w_out, k_cache, v_cache)]
        steps = rows // LOAD_ROWS
        crows = rows // CHUNKS
        hrows = crows // 2
        held = pltpu.VMEM(k_cache.shape, BF16)
        k_all, v_all, k_new, v_new, y = pl.pallas_call(
            functools.partial(step_kernel, group),
            out_shape=(held, held, shape((rows, dim), F32), shape((rows, dim), F32), shape((batch, dim), BF16)),
            in_specs=[HBM] * 8,
            out_specs=[VMEM] * 5,
            scratch_shapes=[
                pltpu.SMEM((batch,), jnp.int32), pltpu.VMEM((1, batch), jnp.int32),
                pltpu.VMEM((batch, embed), BF16), pltpu.VMEM((embed, dim), BF16), pltpu.VMEM((embed, dim), BF16),
                pltpu.VMEM((embed, dim), BF16), pltpu.VMEM(w_out.shape, BF16),
                pltpu.VMEM((batch, dim // 2), F32), pltpu.VMEM((batch, dim // 2), F32), pltpu.VMEM((batch, dim), BF16),
                pltpu.VMEM((group, rows, dim), BF16), pltpu.VMEM((2, group * (rows + 1), LANES), F32),
                pltpu.VMEM((2, group * (crows + 1), LANES), F32), pltpu.VMEM((CHUNKS, 2, group, hrows, dim), BF16),
                pltpu.VMEM((CHUNKS, 2, group, hrows, dim), BF16), pltpu.VMEM(w_out.shape, BF16),
                pltpu.VMEM((CHUNKS, group, group * hrows, dim), BF16),
                pltpu.VMEM((CHUNKS, 2, group // 2, group * hrows, dim), BF16), pltpu.VMEM((batch, dim), F32),
                dma((7,)), dma((steps,)), dma((steps,)), dma((group,)), dma((group,)), dma, dma,
                dma((CHUNKS, group)), dma((CHUNKS, group)), dma((CHUNKS, group)), dma((CHUNKS, group)),
            ],
            compiler_params=pltpu.CompilerParams(collective_id=0, has_side_effects=True, vmem_limit_bytes=14 * mib),
        )(*hbm)
        k_all, v_all = (pltpu.with_memory_space_constraint(x, pltpu.VMEM) for x in (k_all, v_all))
        k_out, v_out, y, _, _ = pl.pallas_call(
            store_kernel,
            out_shape=(shape(k_cache.shape, BF16), shape(k_cache.shape, BF16), shape((batch, dim), BF16), held, held),
            in_specs=[HBM] + [VMEM] * 5,
            out_specs=[HBM, HBM, VMEM, VMEM, VMEM],
            input_output_aliases={1: 3, 2: 4},
            scratch_shapes=[pltpu.SMEM((batch,), jnp.int32), dma, dma((steps,)), dma((steps,))],
            compiler_params=pltpu.CompilerParams(vmem_limit_bytes=4 * mib),
        )(hbm[0], k_all, v_all, k_new, v_new, y)
        return y, k_out, v_out

    return jax.shard_map(
        local_step,
        mesh=mesh,
        in_specs=(P('dp', None), P(None, 'tp'), P(), P(), P('tp', None), cache_spec, cache_spec, P('dp')),
        out_specs=(P('dp', 'tp'), cache_spec, cache_spec),
        check_vma=False,
    )
```

```python
import functools
import math

import jax
import jax.numpy as jnp
from jax import lax
from jax.experimental import pallas as pl
from jax.experimental.pallas import tpu as pltpu
from jax.sharding import PartitionSpec as P

F32, BF16 = jnp.float32, jnp.bfloat16
HBM = pl.BlockSpec(memory_space=pltpu.HBM)
VMEM = pl.BlockSpec(memory_space=pltpu.VMEM)
LOAD_ROWS = 8
CHUNKS = 4
EARLY = 4
PATCH = 16
LANES = 128
GROUP = 4
Q_PARTS = 2


def mm(a, b):
    return jnp.dot(a, b, preferred_element_type=F32)


def rope(x, cosines, sines):
    half = x.shape[-1] // 2
    x1, x2 = x[:, :half], x[:, half:]
    return jnp.concatenate([x1 * cosines - x2 * sines, x2 * cosines + x1 * sines], axis=-1)


def step_kernel(group, lens_h, hid_h, wq_h, wk_h, wv_h, wo_h, k_h, v_h,
                k_o, v_o, kn_o, vn_o, y_o,
                lens_s, lens_v, hid, wq, wk, wv, wo, cosr, sinr, qrot, qbuf, qf, of, ob, obuf, wsib, psend, ybuf, yf,
                h_sem, k_sem, v_sem, q_s, q_r, w_s, w_r, o_s, o_r, y_s, y_r):
    rows, seq, dim = k_o.shape
    batch = hid.shape[0]
    heads = group
    me = lax.axis_index('tp')
    chip, core = lax.div(me, 2), lax.rem(me, 2)
    start = me * rows
    own = pl.ds(start, rows)
    crows = rows // CHUNKS
    hrows = crows // 2
    scale = dim ** -0.5

    def remote(src, dst, ss, rs, peer):
        return pltpu.make_async_remote_copy(src_ref=src, dst_ref=dst, send_sem=ss, recv_sem=rs,
                                            device_id={'tp': peer}, device_id_type=pl.DeviceIdType.MESH)

    def other(d):
        return lax.rem(me + d, group)

    def load(src, dst, sem, i):
        part = pl.ds(i * LOAD_ROWS, LOAD_ROWS)
        return pltpu.make_async_copy(src.at[part], dst.at[part], sem.at[i])

    barrier = pltpu.get_barrier_semaphore()
    for d in range(1, group):
        pl.semaphore_signal(barrier, inc=1, device_id={'tp': other(d)}, device_id_type=pl.DeviceIdType.MESH)
    first = [pltpu.make_async_copy(s, d, h_sem.at[i]) for i, (s, d) in enumerate(
        ((hid_h, hid), (wq_h, wq), (lens_h, lens_v), (lens_h.at[0], lens_s)))]
    later = [pltpu.make_async_copy(s, d, h_sem.at[4 + i]) for i, (s, d) in enumerate(
        ((wk_h, wk), (wv_h, wv), (wo_h, wo)))]
    for copy in first + later:
        copy.start()
    first[2].wait()
    first[3].wait()
    pos = jnp.broadcast_to(lens_v[...].astype(F32), (dim // 2, batch)).T
    freq = jnp.exp(lax.broadcasted_iota(jnp.int32, (1, dim // 2), 1).astype(F32) * (-2.0 * math.log(10000.0) / dim))
    angles = pos * freq
    cosr[...] = jnp.cos(angles)
    sinr[...] = jnp.sin(angles)
    first[0].wait()
    first[1].wait()
    for i in range(EARLY):
        load(k_h, k_o, k_sem, i).start()
        load(v_h, v_o, v_sem, i).start()
    q = mm(hid[...], wq[...]).astype(BF16).astype(F32)
    qrot[...] = rope(q, cosr[...], sinr[...]).astype(BF16)
    pl.semaphore_wait(barrier, group - 1)

    qrows = rows // Q_PARTS
    sends = []
    for part in range(Q_PARTS):
        sends.append([])
        for d in range(1, group):
            peer = other(d)
            copy = remote(qrot.at[pl.ds(peer * rows + part * qrows, qrows)], qbuf.at[me, pl.ds(part * qrows, qrows)],
                          q_s.at[part, d], q_r.at[part, d], peer)
            copy.start()
            sends[-1].append(copy)
    qbuf[me] = qrot[own, :]
    for copy in later:
        copy.wait()
    wcopy = remote(wo, wsib, w_s, w_r, chip * 2 + 1 - core)
    wcopy.start()
    mine = hid[own, :]
    k = mm(mine, wk[...]).astype(BF16).astype(F32)
    kn_o[...] = rope(k, cosr[own, :], sinr[own, :]).astype(BF16).astype(F32)
    vn_o[...] = mm(mine, wv[...]).astype(BF16).astype(F32)

    def take_q(part):
        for copy in sends[part]:
            copy.wait()
        for h in range(heads):
            for lane in range(2):
                qf[lane, pl.ds(h * (rows + 1) + part * qrows, qrows), :] = qbuf[
                    h, pl.ds(part * qrows, qrows), lane * LANES:(lane + 1) * LANES].astype(F32)

    take_q(0)
    for i in range(EARLY, rows // LOAD_ROWS):
        load(k_h, k_o, k_sem, i).start()
        load(v_h, v_o, v_sem, i).start()
    slot = lax.broadcasted_iota(jnp.int32, (heads, seq), 1)

    def scores(b):
        n = lens_s[start + b]
        q = jnp.concatenate([qf[lane, pl.ds(b, heads, stride=rows + 1), :] for lane in range(2)], axis=-1)
        s = lax.dot_general(q.astype(BF16), k_o[b], (((1,), (1,)), ((), ())), preferred_element_type=F32) * scale
        s_new = jnp.sum(q * kn_o[pl.ds(b, 1), :], axis=-1, keepdims=True) * scale
        return jnp.where(slot < n, s, -1e30), s_new

    def softmax(s, s_new):
        top = jnp.maximum(jnp.max(s, axis=-1, keepdims=True), s_new)
        e, e_new = jnp.exp(s - top), jnp.exp(s_new - top)
        return e.astype(BF16), e_new.astype(BF16).astype(F32), jnp.sum(e, axis=-1, keepdims=True) + e_new

    def attend(first_row, crow):
        groups = [range(g, g + GROUP) for g in range(0, crow, GROUP)]
        ready = None
        for g in range(len(groups) + 1):
            nxt = [scores(first_row + u) for u in groups[g]] if g < len(groups) else None
            if ready is not None:
                soft = [softmax(*pair) for pair in ready]
                outs = [mm(e, v_o[first_row + u]) for (e, _, _), u in zip(soft, groups[g - 1])]
                for o, (_, e_new, total), u in zip(outs, soft, groups[g - 1]):
                    o = (o + e_new * vn_o[pl.ds(first_row + u, 1), :]) / total
                    for lane in range(2):
                        of[lane, pl.ds(u, heads, stride=crow + 1), :] = o[:, lane * LANES:(lane + 1) * LANES]
            ready = nxt

    ocopies, ycopies = [], []

    def attend_chunk(ch):
        for step in range(ch * crows // LOAD_ROWS, (ch + 1) * crows // LOAD_ROWS):
            load(k_h, k_o, k_sem, step).wait()
            load(v_h, v_o, v_sem, step).wait()
        attend(ch * crows, crows)
        for h in range(heads):
            for half in range(2):
                part = pl.ds(h * (crows + 1) + half * hrows, hrows)
                ob[ch, half, h] = jnp.concatenate([of[lane, part, :] for lane in range(2)], axis=-1).astype(BF16)
        copies = []
        for d in range(1, group):
            peer = other(d)
            pc, ph = lax.div(peer, 2), lax.rem(peer, 2)
            copy = remote(ob.at[ch, ph, pl.ds(pc * 2, 2)], obuf.at[ch, :, me], o_s.at[ch, d], o_r.at[ch, d], peer)
            copy.start()
            copies.append(copy)
        for p in range(2):
            obuf[ch, p, me] = ob[ch, core, chip * 2 + p]
        ocopies.append(copies)

    def project_chunk(ch):
        for copy in ocopies[ch]:
            copy.wait()
        o_own, o_sib = (obuf[ch, p].astype(F32).reshape(heads * hrows, dim).astype(BF16) for p in (core, 1 - core))
        copies = []
        for d in list(range(1, group)) + [0]:
            peer = other(d)
            cols = pl.ds(pl.multiple_of(peer * dim, dim), dim)
            part = (mm(o_own, wo[:, cols]) + mm(o_sib, wsib[:, cols])).astype(BF16)
            if d:
                psend[ch, d] = part
                copy = remote(psend.at[ch, d], ybuf.at[ch, core, chip], y_s.at[ch, d], y_r.at[ch, d], peer)
                copy.start()
                copies.append(copy)
            else:
                ybuf[ch, core, chip] = part
        ycopies.append(copies)

    def sum_chunk(ch):
        for copy in ycopies[ch]:
            copy.wait()
        for h in range(2):
            total = ybuf[ch, h, 0].astype(F32)
            for c in range(1, group // 2):
                total = total + ybuf[ch, h, c].astype(F32)
            for s in range(group):
                yf[pl.ds(s * rows + ch * crows + h * hrows, hrows), :] = total[s * hrows:(s + 1) * hrows]

    for ch in range(CHUNKS):
        if ch and (ch * crows) % qrows == 0:
            take_q(ch * crows // qrows)
        attend_chunk(ch)
        if ch == 0:
            wcopy.wait()
        else:
            project_chunk(ch - 1)
    project_chunk(CHUNKS - 1)
    for ch in range(CHUNKS):
        sum_chunk(ch)
    y_o[...] = yf[...].astype(BF16)


def store_kernel(lens_h, k_i, v_i, kn, vn, y_i, k_o, v_o, y_o, k_v, v_v, lens_s, l_sem, k_sem, v_sem, p_sem):
    rows, seq, dim = k_v.shape
    start = lax.axis_index('tp') * rows
    pairs = ((k_v, k_o, k_sem, kn), (v_v, v_o, v_sem, vn))

    def store(pair, i):
        part = pl.ds(i * LOAD_ROWS, LOAD_ROWS)
        return pltpu.make_async_copy(pair[0].at[part], pair[1].at[part], pair[2].at[i])

    lens = pltpu.make_async_copy(lens_h.at[0], lens_s, l_sem)
    lens.start()
    for pair in pairs:
        store(pair, 0).start()
    y_o[...] = y_i[...]
    slot = lax.broadcasted_iota(jnp.int32, (PATCH, dim), 0)
    lens.wait()

    def block(b):
        n = lens_s[start + b]
        base = pl.multiple_of(lax.div(n, PATCH) * PATCH, PATCH)
        return n - base, pl.ds(base, PATCH)

    def patch(pair, b):
        at, part = block(b)
        line = jnp.broadcast_to(pair[3][pl.ds(b, 1), :], (PATCH, dim))
        old = pair[0][b, part, :].astype(F32)
        pair[0][b, part, :] = jnp.where(slot == at, line, old).astype(BF16)

    def late(p, b):
        part = block(b)[1]
        return pltpu.make_async_copy(pairs[p][0].at[b, part], pairs[p][1].at[b, part], p_sem.at[p, b])

    def send(i, carry):
        for pair in pairs:
            for r in range(LOAD_ROWS):
                patch(pair, i * LOAD_ROWS + r)
            store(pair, i).start()
        return carry

    lax.fori_loop(1, rows // LOAD_ROWS, send, 0)
    for p in range(2):
        store(pairs[p], 0).wait()
        for b in range(LOAD_ROWS):
            patch(pairs[p], b)
            late(p, b).start()
    for i in range(1, rows // LOAD_ROWS):
        for pair in pairs:
            store(pair, i).wait()
    for p in range(2):
        for b in range(LOAD_ROWS):
            late(p, b).wait()


def solution(mesh):
    group = mesh.shape['tp']
    cache_spec = P(('dp', 'tp'), None, None)

    def local_step(hidden, w_query, w_key, w_value, w_out, k_cache, v_cache, lengths):
        rows, seq, dim = k_cache.shape
        batch, embed = hidden.shape
        shape = jax.ShapeDtypeStruct
        dma, mib = pltpu.SemaphoreType.DMA, 2 ** 20
        hbm = [pltpu.with_memory_space_constraint(x, pltpu.HBM)
               for x in (lengths.reshape(1, batch), hidden, w_query, w_key, w_value, w_out, k_cache, v_cache)]
        steps = rows // LOAD_ROWS
        crows = rows // CHUNKS
        hrows = crows // 2
        held = pltpu.VMEM(k_cache.shape, BF16)
        k_all, v_all, k_new, v_new, y = pl.pallas_call(
            functools.partial(step_kernel, group),
            out_shape=(held, held, shape((rows, dim), F32), shape((rows, dim), F32), shape((batch, dim), BF16)),
            in_specs=[HBM] * 8,
            out_specs=[VMEM] * 5,
            scratch_shapes=[
                pltpu.SMEM((batch,), jnp.int32), pltpu.VMEM((1, batch), jnp.int32),
                pltpu.VMEM((batch, embed), BF16), pltpu.VMEM((embed, dim), BF16), pltpu.VMEM((embed, dim), BF16),
                pltpu.VMEM((embed, dim), BF16), pltpu.VMEM(w_out.shape, BF16),
                pltpu.VMEM((batch, dim // 2), F32), pltpu.VMEM((batch, dim // 2), F32), pltpu.VMEM((batch, dim), BF16),
                pltpu.VMEM((group, rows, dim), BF16), pltpu.VMEM((2, group * (rows + 1), LANES), F32),
                pltpu.VMEM((2, group * (crows + 1), LANES), F32), pltpu.VMEM((CHUNKS, 2, group, hrows, dim), BF16),
                pltpu.VMEM((CHUNKS, 2, group, hrows, dim), BF16), pltpu.VMEM(w_out.shape, BF16),
                pltpu.VMEM((CHUNKS, group, group * hrows, dim), BF16),
                pltpu.VMEM((CHUNKS, 2, group // 2, group * hrows, dim), BF16), pltpu.VMEM((batch, dim), F32),
                dma((7,)), dma((steps,)), dma((steps,)), dma((Q_PARTS, group)), dma((Q_PARTS, group)), dma, dma,
                dma((CHUNKS, group)), dma((CHUNKS, group)), dma((CHUNKS, group)), dma((CHUNKS, group)),
            ],
            compiler_params=pltpu.CompilerParams(collective_id=0, has_side_effects=True, vmem_limit_bytes=14 * mib),
        )(*hbm)
        k_all, v_all = (pltpu.with_memory_space_constraint(x, pltpu.VMEM) for x in (k_all, v_all))
        k_out, v_out, y, _, _ = pl.pallas_call(
            store_kernel,
            out_shape=(shape(k_cache.shape, BF16), shape(k_cache.shape, BF16), shape((batch, dim), BF16), held, held),
            in_specs=[HBM] + [VMEM] * 5,
            out_specs=[HBM, HBM, VMEM, VMEM, VMEM],
            input_output_aliases={1: 3, 2: 4},
            scratch_shapes=[pltpu.SMEM((batch,), jnp.int32), dma, dma((steps,)), dma((steps,)), dma((2, LOAD_ROWS))],
            compiler_params=pltpu.CompilerParams(vmem_limit_bytes=4 * mib),
        )(hbm[0], k_all, v_all, k_new, v_new, y)
        return y, k_out, v_out

    return jax.shard_map(
        local_step,
        mesh=mesh,
        in_specs=(P('dp', None), P(None, 'tp'), P(), P(), P('tp', None), cache_spec, cache_spec, P('dp')),
        out_specs=(P('dp', 'tp'), cache_spec, cache_spec),
        check_vma=False,
    )
```

```python
import functools
import math

import jax
import jax.numpy as jnp
from jax import lax
from jax.experimental import pallas as pl
from jax.experimental.pallas import tpu as pltpu
from jax.sharding import PartitionSpec as P

F32, BF16 = jnp.float32, jnp.bfloat16
HBM = pl.BlockSpec(memory_space=pltpu.HBM)
VMEM = pl.BlockSpec(memory_space=pltpu.VMEM)
LOAD_ROWS = 8
CHUNKS = 4
EARLY = 4
PATCH = 16
LANES = 128
GROUP = 4
Q_PARTS = 2


def mm(a, b):
    return jnp.dot(a, b, preferred_element_type=F32)


def rope(x, cosines, sines):
    half = x.shape[-1] // 2
    x1, x2 = x[:, :half], x[:, half:]
    return jnp.concatenate([x1 * cosines - x2 * sines, x2 * cosines + x1 * sines], axis=-1)


def step_kernel(group, lens_h, hid_h, wq_h, wk_h, wv_h, wo_h, k_h, v_h,
                k_o, v_o, kn_o, vn_o, y_o,
                lens_s, lens_v, hid, wq, wk, wv, wo, cosr, sinr, qrot, qbuf, qf, of, ob, obuf, wsib, psend, ybuf, rel, yf,
                h_sem, k_sem, v_sem, q_s, q_r, w_s, w_r, o_s, o_r, y_s, y_r, r_r):
    rows, seq, dim = k_o.shape
    batch = hid.shape[0]
    heads = group
    me = lax.axis_index('tp')
    chip, core = lax.div(me, 2), lax.rem(me, 2)
    start = me * rows
    own = pl.ds(start, rows)
    crows = rows // CHUNKS
    hrows = crows // 2
    scale = dim ** -0.5

    def remote(src, dst, ss, rs, peer):
        return pltpu.make_async_remote_copy(src_ref=src, dst_ref=dst, send_sem=ss, recv_sem=rs,
                                            device_id={'tp': peer}, device_id_type=pl.DeviceIdType.MESH)

    def other(d):
        return lax.rem(me + d, group)

    def load(src, dst, sem, i):
        part = pl.ds(i * LOAD_ROWS, LOAD_ROWS)
        return pltpu.make_async_copy(src.at[part], dst.at[part], sem.at[i])

    barrier = pltpu.get_barrier_semaphore()
    for d in range(1, group):
        pl.semaphore_signal(barrier, inc=1, device_id={'tp': other(d)}, device_id_type=pl.DeviceIdType.MESH)
    first = [pltpu.make_async_copy(s, d, h_sem.at[i]) for i, (s, d) in enumerate(
        ((hid_h, hid), (wq_h, wq), (lens_h, lens_v), (lens_h.at[0], lens_s)))]
    later = [pltpu.make_async_copy(s, d, h_sem.at[4 + i]) for i, (s, d) in enumerate(
        ((wk_h, wk), (wv_h, wv), (wo_h, wo)))]
    for copy in first + later:
        copy.start()
    first[2].wait()
    first[3].wait()
    pos = jnp.broadcast_to(lens_v[...].astype(F32), (dim // 2, batch)).T
    freq = jnp.exp(lax.broadcasted_iota(jnp.int32, (1, dim // 2), 1).astype(F32) * (-2.0 * math.log(10000.0) / dim))
    angles = pos * freq
    cosr[...] = jnp.cos(angles)
    sinr[...] = jnp.sin(angles)
    first[0].wait()
    first[1].wait()
    for i in range(EARLY):
        load(k_h, k_o, k_sem, i).start()
        load(v_h, v_o, v_sem, i).start()
    q = mm(hid[...], wq[...]).astype(BF16).astype(F32)
    qrot[...] = rope(q, cosr[...], sinr[...]).astype(BF16)
    pl.semaphore_wait(barrier, group - 1)

    qrows = rows // Q_PARTS
    sends = []
    for part in range(Q_PARTS):
        sends.append([])
        for d in range(1, group):
            peer = other(d)
            copy = remote(qrot.at[pl.ds(peer * rows + part * qrows, qrows)], qbuf.at[me, pl.ds(part * qrows, qrows)],
                          q_s.at[part, d], q_r.at[part, d], peer)
            copy.start()
            sends[-1].append(copy)
    qbuf[me] = qrot[own, :]
    for copy in later:
        copy.wait()
    wcopy = remote(wo, wsib, w_s, w_r, chip * 2 + 1 - core)
    wcopy.start()
    mine = hid[own, :]
    k = mm(mine, wk[...]).astype(BF16).astype(F32)
    kn_o[...] = rope(k, cosr[own, :], sinr[own, :]).astype(BF16).astype(F32)
    vn_o[...] = mm(mine, wv[...]).astype(BF16).astype(F32)

    def take_q(part):
        for copy in sends[part]:
            copy.wait()
        for h in range(heads):
            for lane in range(2):
                qf[lane, pl.ds(h * (rows + 1) + part * qrows, qrows), :] = qbuf[
                    h, pl.ds(part * qrows, qrows), lane * LANES:(lane + 1) * LANES].astype(F32)

    take_q(0)
    for i in range(EARLY, rows // LOAD_ROWS):
        load(k_h, k_o, k_sem, i).start()
        load(v_h, v_o, v_sem, i).start()
    slot = lax.broadcasted_iota(jnp.int32, (heads, seq), 1)

    def scores(b):
        n = lens_s[start + b]
        q = jnp.concatenate([qf[lane, pl.ds(b, heads, stride=rows + 1), :] for lane in range(2)], axis=-1)
        s = lax.dot_general(q.astype(BF16), k_o[b], (((1,), (1,)), ((), ())), preferred_element_type=F32) * scale
        s_new = jnp.sum(q * kn_o[pl.ds(b, 1), :], axis=-1, keepdims=True) * scale
        return jnp.where(slot < n, s, -1e30), s_new

    def softmax(s, s_new):
        top = jnp.maximum(jnp.max(s, axis=-1, keepdims=True), s_new)
        e, e_new = jnp.exp(s - top), jnp.exp(s_new - top)
        return e.astype(BF16), e_new.astype(BF16).astype(F32), jnp.sum(e, axis=-1, keepdims=True) + e_new

    def attend(first_row, crow):
        groups = [range(g, g + GROUP) for g in range(0, crow, GROUP)]
        ready = None
        for g in range(len(groups) + 1):
            nxt = [scores(first_row + u) for u in groups[g]] if g < len(groups) else None
            if ready is not None:
                soft = [softmax(*pair) for pair in ready]
                outs = [mm(e, v_o[first_row + u]) for (e, _, _), u in zip(soft, groups[g - 1])]
                for o, (_, e_new, total), u in zip(outs, soft, groups[g - 1]):
                    o = (o + e_new * vn_o[pl.ds(first_row + u, 1), :]) / total
                    for lane in range(2):
                        of[lane, pl.ds(u, heads, stride=crow + 1), :] = o[:, lane * LANES:(lane + 1) * LANES]
            ready = nxt

    ocopies, ycopies = [], []

    def attend_chunk(ch):
        for step in range(ch * crows // LOAD_ROWS, (ch + 1) * crows // LOAD_ROWS):
            load(k_h, k_o, k_sem, step).wait()
            load(v_h, v_o, v_sem, step).wait()
        attend(ch * crows, crows)
        for h in range(heads):
            for half in range(2):
                part = pl.ds(h * (crows + 1) + half * hrows, hrows)
                ob[ch, half, h] = jnp.concatenate([of[lane, part, :] for lane in range(2)], axis=-1).astype(BF16)
        copies = []
        for d in range(1, group):
            peer = other(d)
            pc, ph = lax.div(peer, 2), lax.rem(peer, 2)
            copy = remote(ob.at[ch, ph, pl.ds(pc * 2, 2)], obuf.at[ch, :, me], o_s.at[ch, d], o_r.at[ch, d], peer)
            copy.start()
            copies.append(copy)
        for p in range(2):
            obuf[ch, p, me] = ob[ch, core, chip * 2 + p]
        ocopies.append(copies)

    x, y = lax.rem(chip, 2), lax.div(chip, 2)

    def device(dy, dx, k):
        return (y + dy - 2 * y * dy) * 4 + (x + dx - 2 * x * dx) * 2 + k

    def partial(ch, peer):
        o_own, o_sib = (obuf[ch, p].astype(F32).reshape(heads * hrows, dim).astype(BF16) for p in (core, 1 - core))
        cols = pl.ds(pl.multiple_of(peer * dim, dim), dim)
        return mm(o_own, wo[:, cols]) + mm(o_sib, wsib[:, cols])

    relays = []

    def push(ch, i, value, dst, sem, peer):
        psend[ch, i] = value.astype(BF16)
        copy = remote(psend.at[ch, i], dst, y_s.at[ch, i], sem, peer)
        copy.start()
        return copy

    def project_chunk(ch):
        for copy in ocopies[ch]:
            copy.wait()
        relays.append([
            push(ch, 0, partial(ch, device(1, 1, 0)), rel.at[ch, 0], r_r.at[ch, 0], device(0, 1, core)),
            push(ch, 1, partial(ch, device(1, 1, 1)), rel.at[ch, 1], r_r.at[ch, 1], device(1, 0, core))])
        ycopies.append([
            push(ch, 2, partial(ch, device(0, 1, 0)), ybuf.at[ch, core, 1], y_r.at[ch, 1, core], device(0, 1, 0)),
            push(ch, 3, partial(ch, device(1, 0, 1)), ybuf.at[ch, core, 2], y_r.at[ch, 2, core], device(1, 0, 1)),
            push(ch, 4, partial(ch, device(0, 0, 1 - core)), ybuf.at[ch, core, 0], y_r.at[ch, 0, core],
                 device(0, 0, 1 - core))])
        ybuf[ch, core, 0] = partial(ch, me).astype(BF16)

    def relay_chunk(ch):
        for i, peer, slot in ((0, device(1, 0, 0), 2), (1, device(0, 1, 1), 1)):
            mine = partial(ch, peer)
            relays[ch][i].wait()
            ycopies[ch].append(push(ch, 5 + i, mine + rel[ch, i].astype(F32), ybuf.at[ch, core, slot],
                                    y_r.at[ch, slot, core], peer))

    def sum_chunk(ch):
        def arrived(h, part):
            remote(ybuf.at[ch, h, part], ybuf.at[ch, h, part], y_s.at[ch, 4], y_r.at[ch, part, h], me).wait_recv()

        for copy in ycopies[ch]:
            copy.wait_send()
        arrived(1 - core, 0)
        for h in range(2):
            arrived(h, 1)
            arrived(h, 2)
        for h in range(2):
            total = ybuf[ch, h, 0].astype(F32) + ybuf[ch, h, 1].astype(F32) + ybuf[ch, h, 2].astype(F32)
            for s in range(group):
                yf[pl.ds(s * rows + ch * crows + h * hrows, hrows), :] = total[s * hrows:(s + 1) * hrows]

    for ch in range(CHUNKS):
        if ch and (ch * crows) % qrows == 0:
            take_q(ch * crows // qrows)
        attend_chunk(ch)
        if ch == 0:
            wcopy.wait()
        else:
            project_chunk(ch - 1)
        if ch > 1:
            relay_chunk(ch - 2)
    project_chunk(CHUNKS - 1)
    relay_chunk(CHUNKS - 2)
    relay_chunk(CHUNKS - 1)
    for ch in range(CHUNKS):
        sum_chunk(ch)
    y_o[...] = yf[...].astype(BF16)


def store_kernel(lens_h, k_i, v_i, kn, vn, y_i, k_o, v_o, y_o, k_v, v_v, lens_s, l_sem, k_sem, v_sem, p_sem):
    rows, seq, dim = k_v.shape
    start = lax.axis_index('tp') * rows
    pairs = ((k_v, k_o, k_sem, kn), (v_v, v_o, v_sem, vn))

    def store(pair, i):
        part = pl.ds(i * LOAD_ROWS, LOAD_ROWS)
        return pltpu.make_async_copy(pair[0].at[part], pair[1].at[part], pair[2].at[i])

    lens = pltpu.make_async_copy(lens_h.at[0], lens_s, l_sem)
    lens.start()
    for pair in pairs:
        store(pair, 0).start()
    y_o[...] = y_i[...]
    slot = lax.broadcasted_iota(jnp.int32, (PATCH, dim), 0)
    lens.wait()

    def block(b):
        n = lens_s[start + b]
        base = pl.multiple_of(lax.div(n, PATCH) * PATCH, PATCH)
        return n - base, pl.ds(base, PATCH)

    def patch(pair, b):
        at, part = block(b)
        line = jnp.broadcast_to(pair[3][pl.ds(b, 1), :], (PATCH, dim))
        old = pair[0][b, part, :].astype(F32)
        pair[0][b, part, :] = jnp.where(slot == at, line, old).astype(BF16)

    def late(p, b):
        part = block(b)[1]
        return pltpu.make_async_copy(pairs[p][0].at[b, part], pairs[p][1].at[b, part], p_sem.at[p, b])

    def send(i, carry):
        for pair in pairs:
            for r in range(LOAD_ROWS):
                patch(pair, i * LOAD_ROWS + r)
            store(pair, i).start()
        return carry

    lax.fori_loop(1, rows // LOAD_ROWS, send, 0)
    for p in range(2):
        store(pairs[p], 0).wait()
        for b in range(LOAD_ROWS):
            patch(pairs[p], b)
            late(p, b).start()
    for i in range(1, rows // LOAD_ROWS):
        for pair in pairs:
            store(pair, i).wait()
    for p in range(2):
        for b in range(LOAD_ROWS):
            late(p, b).wait()


def solution(mesh):
    group = mesh.shape['tp']
    cache_spec = P(('dp', 'tp'), None, None)

    def local_step(hidden, w_query, w_key, w_value, w_out, k_cache, v_cache, lengths):
        rows, seq, dim = k_cache.shape
        batch, embed = hidden.shape
        shape = jax.ShapeDtypeStruct
        dma, mib = pltpu.SemaphoreType.DMA, 2 ** 20
        hbm = [pltpu.with_memory_space_constraint(x, pltpu.HBM)
               for x in (lengths.reshape(1, batch), hidden, w_query, w_key, w_value, w_out, k_cache, v_cache)]
        steps = rows // LOAD_ROWS
        crows = rows // CHUNKS
        hrows = crows // 2
        held = pltpu.VMEM(k_cache.shape, BF16)
        k_all, v_all, k_new, v_new, y = pl.pallas_call(
            functools.partial(step_kernel, group),
            out_shape=(held, held, shape((rows, dim), F32), shape((rows, dim), F32), shape((batch, dim), BF16)),
            in_specs=[HBM] * 8,
            out_specs=[VMEM] * 5,
            scratch_shapes=[
                pltpu.SMEM((batch,), jnp.int32), pltpu.VMEM((1, batch), jnp.int32),
                pltpu.VMEM((batch, embed), BF16), pltpu.VMEM((embed, dim), BF16), pltpu.VMEM((embed, dim), BF16),
                pltpu.VMEM((embed, dim), BF16), pltpu.VMEM(w_out.shape, BF16),
                pltpu.VMEM((batch, dim // 2), F32), pltpu.VMEM((batch, dim // 2), F32), pltpu.VMEM((batch, dim), BF16),
                pltpu.VMEM((group, rows, dim), BF16), pltpu.VMEM((2, group * (rows + 1), LANES), F32),
                pltpu.VMEM((2, group * (crows + 1), LANES), F32), pltpu.VMEM((CHUNKS, 2, group, hrows, dim), BF16),
                pltpu.VMEM((CHUNKS, 2, group, hrows, dim), BF16), pltpu.VMEM(w_out.shape, BF16),
                pltpu.VMEM((CHUNKS, 7, group * hrows, dim), BF16),
                pltpu.VMEM((CHUNKS, 2, 3, group * hrows, dim), BF16), pltpu.VMEM((CHUNKS, 2, group * hrows, dim), BF16),
                pltpu.VMEM((batch, dim), F32),
                dma((7,)), dma((steps,)), dma((steps,)), dma((Q_PARTS, group)), dma((Q_PARTS, group)), dma, dma,
                dma((CHUNKS, group)), dma((CHUNKS, group)), dma((CHUNKS, 7)), dma((CHUNKS, 3, 2)), dma((CHUNKS, 2)),
            ],
            compiler_params=pltpu.CompilerParams(collective_id=0, has_side_effects=True, vmem_limit_bytes=14 * mib),
        )(*hbm)
        k_all, v_all = (pltpu.with_memory_space_constraint(x, pltpu.VMEM) for x in (k_all, v_all))
        k_out, v_out, y, _, _ = pl.pallas_call(
            store_kernel,
            out_shape=(shape(k_cache.shape, BF16), shape(k_cache.shape, BF16), shape((batch, dim), BF16), held, held),
            in_specs=[HBM] + [VMEM] * 5,
            out_specs=[HBM, HBM, VMEM, VMEM, VMEM],
            input_output_aliases={1: 3, 2: 4},
            scratch_shapes=[pltpu.SMEM((batch,), jnp.int32), dma, dma((steps,)), dma((steps,)), dma((2, LOAD_ROWS))],
            compiler_params=pltpu.CompilerParams(vmem_limit_bytes=4 * mib),
        )(hbm[0], k_all, v_all, k_new, v_new, y)
        return y, k_out, v_out

    return jax.shard_map(
        local_step,
        mesh=mesh,
        in_specs=(P('dp', None), P(None, 'tp'), P(), P(), P('tp', None), cache_spec, cache_spec, P('dp')),
        out_specs=(P('dp', 'tp'), cache_spec, cache_spec),
        check_vma=False,
    )
```

```python
import functools
import math

import jax
import jax.numpy as jnp
from jax import lax
from jax.experimental import pallas as pl
from jax.experimental.pallas import tpu as pltpu
from jax.sharding import PartitionSpec as P

F32, BF16 = jnp.float32, jnp.bfloat16
HBM = pl.BlockSpec(memory_space=pltpu.HBM)
VMEM = pl.BlockSpec(memory_space=pltpu.VMEM)
LOAD_ROWS = 8
CHUNKS = 4
EARLY = 4
PATCH = 16
LANES = 128
GROUP = 4
Q_PARTS = 2


def mm(a, b):
    return jnp.dot(a, b, preferred_element_type=F32)


def rope(x, cosines, sines):
    half = x.shape[-1] // 2
    x1, x2 = x[:, :half], x[:, half:]
    return jnp.concatenate([x1 * cosines - x2 * sines, x2 * cosines + x1 * sines], axis=-1)


def step_kernel(group, lens_h, hid_h, wq_h, wk_h, wv_h, wo_h, k_h, v_h,
                k_o, v_o, kn_o, vn_o, y_o,
                lens_s, lens_v, hid, wq, wk, wv, wo, cosr, sinr, qrot, qbuf, qf, of, ob, obuf, wsib, psend, ybuf, yf,
                h_sem, k_sem, v_sem, q_s, q_r, w_s, w_r, o_s, o_r, y_s, y_r):
    rows, seq, dim = k_o.shape
    batch = hid.shape[0]
    heads = group
    me = lax.axis_index('tp')
    chip, core = lax.div(me, 2), lax.rem(me, 2)
    start = me * rows
    own = pl.ds(start, rows)
    crows = rows // CHUNKS
    hrows = crows // 2
    scale = dim ** -0.5

    def remote(src, dst, ss, rs, peer):
        return pltpu.make_async_remote_copy(src_ref=src, dst_ref=dst, send_sem=ss, recv_sem=rs,
                                            device_id={'tp': peer}, device_id_type=pl.DeviceIdType.MESH)

    def other(d):
        return lax.rem(me + d, group)

    def load(src, dst, sem, i):
        part = pl.ds(i * LOAD_ROWS, LOAD_ROWS)
        return pltpu.make_async_copy(src.at[part], dst.at[part], sem.at[i])

    barrier = pltpu.get_barrier_semaphore()
    for d in range(1, group):
        pl.semaphore_signal(barrier, inc=1, device_id={'tp': other(d)}, device_id_type=pl.DeviceIdType.MESH)
    first = [pltpu.make_async_copy(s, d, h_sem.at[i]) for i, (s, d) in enumerate(
        ((hid_h, hid), (wq_h, wq), (lens_h, lens_v), (lens_h.at[0], lens_s)))]
    later = [pltpu.make_async_copy(s, d, h_sem.at[4 + i]) for i, (s, d) in enumerate(
        ((wk_h, wk), (wv_h, wv), (wo_h, wo)))]
    for copy in first:
        copy.start()
    first[2].wait()
    first[3].wait()
    for copy in later:
        copy.start()
    pos = jnp.broadcast_to(lens_v[...].astype(F32), (dim // 2, batch)).T
    freq = jnp.exp(lax.broadcasted_iota(jnp.int32, (1, dim // 2), 1).astype(F32) * (-2.0 * math.log(10000.0) / dim))
    angles = pos * freq
    cosr[...] = jnp.cos(angles)
    sinr[...] = jnp.sin(angles)
    first[0].wait()
    first[1].wait()
    for i in range(EARLY):
        load(k_h, k_o, k_sem, i).start()
        load(v_h, v_o, v_sem, i).start()
    q = mm(hid[...], wq[...]).astype(BF16).astype(F32)
    qrot[...] = rope(q, cosr[...], sinr[...]).astype(BF16)
    pl.semaphore_wait(barrier, group - 1)

    qrows = rows // Q_PARTS
    sends = []
    for part in range(Q_PARTS):
        sends.append([])
        for d in range(1, group):
            peer = other(d)
            copy = remote(qrot.at[pl.ds(peer * rows + part * qrows, qrows)], qbuf.at[me, pl.ds(part * qrows, qrows)],
                          q_s.at[part, d], q_r.at[part, d], peer)
            copy.start()
            sends[-1].append(copy)
    qbuf[me] = qrot[own, :]
    for copy in later:
        copy.wait()
    wcopy = remote(wo, wsib, w_s, w_r, chip * 2 + 1 - core)
    wcopy.start()
    mine = hid[own, :]
    k = mm(mine, wk[...]).astype(BF16).astype(F32)
    kn_o[...] = rope(k, cosr[own, :], sinr[own, :]).astype(BF16).astype(F32)
    vn_o[...] = mm(mine, wv[...]).astype(BF16).astype(F32)

    def take_q(part):
        for copy in sends[part]:
            copy.wait()
        for h in range(heads):
            for lane in range(2):
                qf[lane, pl.ds(h * (rows + 1) + part * qrows, qrows), :] = qbuf[
                    h, pl.ds(part * qrows, qrows), lane * LANES:(lane + 1) * LANES].astype(F32)

    for i in range(EARLY):
        load(k_h, k_o, k_sem, i).wait()
        load(v_h, v_o, v_sem, i).wait()
    for i in range(EARLY, rows // LOAD_ROWS):
        load(k_h, k_o, k_sem, i).start()
        load(v_h, v_o, v_sem, i).start()
    slot = lax.broadcasted_iota(jnp.int32, (heads, seq), 1)

    def scores(b):
        n = lens_s[start + b]
        q = jnp.concatenate([qf[lane, pl.ds(b, heads, stride=rows + 1), :] for lane in range(2)], axis=-1)
        s = lax.dot_general(q.astype(BF16), k_o[b], (((1,), (1,)), ((), ())), preferred_element_type=F32) * scale
        s_new = jnp.sum(q * kn_o[pl.ds(b, 1), :], axis=-1, keepdims=True) * scale
        return jnp.where(slot < n, s, -1e30), s_new

    def softmax(s, s_new):
        top = jnp.maximum(jnp.max(s, axis=-1, keepdims=True), s_new)
        e, e_new = jnp.exp(s - top), jnp.exp(s_new - top)
        return e.astype(BF16), e_new.astype(BF16).astype(F32), jnp.sum(e, axis=-1, keepdims=True) + e_new

    def value(b, row, e, e_new, total):
        o = (mm(e, v_o[b]) + e_new * vn_o[pl.ds(b, 1), :]) / total
        return row, o

    def keep(row, o):
        for lane in range(2):
            of[lane, pl.ds(row, heads, stride=crows + 1), :] = o[:, lane * LANES:(lane + 1) * LANES]

    ocopies, ycopies = [], []

    def begin_chunk(ch):
        if (ch * crows) % qrows == 0:
            take_q(ch * crows // qrows)
        for step in range(max(EARLY, ch * crows // LOAD_ROWS), (ch + 1) * crows // LOAD_ROWS):
            load(k_h, k_o, k_sem, step).wait()
            load(v_h, v_o, v_sem, step).wait()

    def send_chunk(ch):
        for h in range(heads):
            for half in range(2):
                part = pl.ds(h * (crows + 1) + half * hrows, hrows)
                ob[ch, half, h] = jnp.concatenate([of[lane, part, :] for lane in range(2)], axis=-1).astype(BF16)
        copies = []
        for d in range(1, group):
            peer = other(d)
            pc, ph = lax.div(peer, 2), lax.rem(peer, 2)
            copy = remote(ob.at[ch, ph, pl.ds(pc * 2, 2)], obuf.at[ch, :, me], o_s.at[ch, d], o_r.at[ch, d], peer)
            copy.start()
            copies.append(copy)
        for p in range(2):
            obuf[ch, p, me] = ob[ch, core, chip * 2 + p]
        ocopies.append(copies)

    def project_chunk(ch):
        for copy in ocopies[ch]:
            copy.wait()
        o_own, o_sib = (obuf[ch, p].astype(F32).reshape(heads * hrows, dim).astype(BF16) for p in (core, 1 - core))
        copies = []
        for d in list(range(1, group)) + [0]:
            peer = other(d)
            cols = pl.ds(pl.multiple_of(peer * dim, dim), dim)
            part = (mm(o_own, wo[:, cols]) + mm(o_sib, wsib[:, cols])).astype(BF16)
            if d:
                psend[ch, d] = part
                copy = remote(psend.at[ch, d], ybuf.at[ch, core, chip], y_s.at[ch, d], y_r.at[ch, d], peer)
                copy.start()
                copies.append(copy)
            else:
                ybuf[ch, core, chip] = part
        ycopies.append(copies)

    def sum_chunk(ch):
        for copy in ycopies[ch]:
            copy.wait()
        for h in range(2):
            total = ybuf[ch, h, 0].astype(F32)
            for c in range(1, group // 2):
                total = total + ybuf[ch, h, c].astype(F32)
            for s in range(group):
                yf[pl.ds(s * rows + ch * crows + h * hrows, hrows), :] = total[s * hrows:(s + 1) * hrows]

    per_chunk = crows // GROUP
    ready = None
    for g in range(CHUNKS * per_chunk + 1):
        ch = g // per_chunk
        if ch < CHUNKS and g % per_chunk == 0:
            begin_chunk(ch)
        nxt = [(b, scores(b)) for b in range(g * GROUP, (g + 1) * GROUP)] if ch < CHUNKS else None
        if ready is not None:
            soft = [(b, softmax(*pair)) for b, pair in ready]
            for row, o in [value(b, b % crows, *parts) for b, parts in soft]:
                keep(row, o)
            if g % per_chunk == 0:
                send_chunk(ch - 1)
                if ch == 1:
                    wcopy.wait()
                else:
                    project_chunk(ch - 2)
        ready = nxt
    project_chunk(CHUNKS - 1)
    for ch in range(CHUNKS):
        sum_chunk(ch)
    y_o[...] = yf[...].astype(BF16)


def store_kernel(lens_h, k_i, v_i, kn, vn, y_i, k_o, v_o, y_o, k_v, v_v, lens_s, l_sem, k_sem, v_sem, p_sem):
    rows, seq, dim = k_v.shape
    start = lax.axis_index('tp') * rows
    pairs = ((k_v, k_o, k_sem, kn), (v_v, v_o, v_sem, vn))

    def store(pair, i):
        part = pl.ds(i * LOAD_ROWS, LOAD_ROWS)
        return pltpu.make_async_copy(pair[0].at[part], pair[1].at[part], pair[2].at[i])

    lens = pltpu.make_async_copy(lens_h.at[0], lens_s, l_sem)
    lens.start()
    for pair in pairs:
        store(pair, 0).start()
    y_o[...] = y_i[...]
    slot = lax.broadcasted_iota(jnp.int32, (PATCH, dim), 0)
    lens.wait()

    def block(b):
        n = lens_s[start + b]
        base = pl.multiple_of(lax.div(n, PATCH) * PATCH, PATCH)
        return n - base, pl.ds(base, PATCH)

    def patch(pair, b):
        at, part = block(b)
        line = jnp.broadcast_to(pair[3][pl.ds(b, 1), :], (PATCH, dim))
        old = pair[0][b, part, :].astype(F32)
        pair[0][b, part, :] = jnp.where(slot == at, line, old).astype(BF16)

    def late(p, b):
        part = block(b)[1]
        return pltpu.make_async_copy(pairs[p][0].at[b, part], pairs[p][1].at[b, part], p_sem.at[p, b])

    def send(i, carry):
        for pair in pairs:
            for r in range(LOAD_ROWS):
                patch(pair, i * LOAD_ROWS + r)
            store(pair, i).start()
        return carry

    lax.fori_loop(1, rows // LOAD_ROWS, send, 0)
    for p in range(2):
        store(pairs[p], 0).wait()
        for b in range(LOAD_ROWS):
            patch(pairs[p], b)
            late(p, b).start()
    for i in range(1, rows // LOAD_ROWS):
        for pair in pairs:
            store(pair, i).wait()
    for p in range(2):
        for b in range(LOAD_ROWS):
            late(p, b).wait()


def solution(mesh):
    group = mesh.shape['tp']
    cache_spec = P(('dp', 'tp'), None, None)

    def local_step(hidden, w_query, w_key, w_value, w_out, k_cache, v_cache, lengths):
        rows, seq, dim = k_cache.shape
        batch, embed = hidden.shape
        shape = jax.ShapeDtypeStruct
        dma, mib = pltpu.SemaphoreType.DMA, 2 ** 20
        hbm = [pltpu.with_memory_space_constraint(x, pltpu.HBM)
               for x in (lengths.reshape(1, batch), hidden, w_query, w_key, w_value, w_out, k_cache, v_cache)]
        steps = rows // LOAD_ROWS
        crows = rows // CHUNKS
        hrows = crows // 2
        held = pltpu.VMEM(k_cache.shape, BF16)
        k_all, v_all, k_new, v_new, y = pl.pallas_call(
            functools.partial(step_kernel, group),
            out_shape=(held, held, shape((rows, dim), F32), shape((rows, dim), F32), shape((batch, dim), BF16)),
            in_specs=[HBM] * 8,
            out_specs=[VMEM] * 5,
            scratch_shapes=[
                pltpu.SMEM((batch,), jnp.int32), pltpu.VMEM((1, batch), jnp.int32),
                pltpu.VMEM((batch, embed), BF16), pltpu.VMEM((embed, dim), BF16), pltpu.VMEM((embed, dim), BF16),
                pltpu.VMEM((embed, dim), BF16), pltpu.VMEM(w_out.shape, BF16),
                pltpu.VMEM((batch, dim // 2), F32), pltpu.VMEM((batch, dim // 2), F32), pltpu.VMEM((batch, dim), BF16),
                pltpu.VMEM((group, rows, dim), BF16), pltpu.VMEM((2, group * (rows + 1), LANES), F32),
                pltpu.VMEM((2, group * (crows + 1), LANES), F32), pltpu.VMEM((CHUNKS, 2, group, hrows, dim), BF16),
                pltpu.VMEM((CHUNKS, 2, group, hrows, dim), BF16), pltpu.VMEM(w_out.shape, BF16),
                pltpu.VMEM((CHUNKS, group, group * hrows, dim), BF16),
                pltpu.VMEM((CHUNKS, 2, group // 2, group * hrows, dim), BF16), pltpu.VMEM((batch, dim), F32),
                dma((7,)), dma((steps,)), dma((steps,)), dma((Q_PARTS, group)), dma((Q_PARTS, group)), dma, dma,
                dma((CHUNKS, group)), dma((CHUNKS, group)), dma((CHUNKS, group)), dma((CHUNKS, group)),
            ],
            compiler_params=pltpu.CompilerParams(collective_id=0, has_side_effects=True, vmem_limit_bytes=14 * mib),
        )(*hbm)
        k_all, v_all = (pltpu.with_memory_space_constraint(x, pltpu.VMEM) for x in (k_all, v_all))
        k_out, v_out, y, _, _ = pl.pallas_call(
            store_kernel,
            out_shape=(shape(k_cache.shape, BF16), shape(k_cache.shape, BF16), shape((batch, dim), BF16), held, held),
            in_specs=[HBM] + [VMEM] * 5,
            out_specs=[HBM, HBM, VMEM, VMEM, VMEM],
            input_output_aliases={1: 3, 2: 4},
            scratch_shapes=[pltpu.SMEM((batch,), jnp.int32), dma, dma((steps,)), dma((steps,)), dma((2, LOAD_ROWS))],
            compiler_params=pltpu.CompilerParams(vmem_limit_bytes=4 * mib),
        )(hbm[0], k_all, v_all, k_new, v_new, y)
        return y, k_out, v_out

    return jax.shard_map(
        local_step,
        mesh=mesh,
        in_specs=(P('dp', None), P(None, 'tp'), P(), P(), P('tp', None), cache_spec, cache_spec, P('dp')),
        out_specs=(P('dp', 'tp'), cache_spec, cache_spec),
        check_vma=False,
    )
```

```python
import functools
import math

import jax
import jax.numpy as jnp
from jax import lax
from jax.experimental import pallas as pl
from jax.experimental.pallas import tpu as pltpu
from jax.sharding import PartitionSpec as P

F32, BF16 = jnp.float32, jnp.bfloat16
HBM = pl.BlockSpec(memory_space=pltpu.HBM)
VMEM = pl.BlockSpec(memory_space=pltpu.VMEM)
LOAD_ROWS = 8
CHUNKS = 4
EARLY = 4
PATCH = 16
LANES = 128
GROUP = 4
Q_PARTS = 2


def mm(a, b):
    return jnp.dot(a, b, preferred_element_type=F32)


def rope(x, cosines, sines):
    half = x.shape[-1] // 2
    x1, x2 = x[:, :half], x[:, half:]
    return jnp.concatenate([x1 * cosines - x2 * sines, x2 * cosines + x1 * sines], axis=-1)


def step_kernel(group, lens_h, hid_h, wq_h, wk_h, wv_h, wo_h, k_h, v_h,
                k_o, v_o, kn_o, vn_o, y_o,
                lens_s, lens_v, hid, wq, wk, wv, wo, cosr, sinr, qrot, qbuf, qf, of, ob, obuf, wsib, psend, ybuf, yf,
                h_sem, k_sem, v_sem, q_s, q_r, w_s, w_r, o_s, o_r, y_s, y_r):
    rows, seq, dim = k_o.shape
    batch = hid.shape[0]
    heads = group
    me = lax.axis_index('tp')
    chip, core = lax.div(me, 2), lax.rem(me, 2)
    start = me * rows
    own = pl.ds(start, rows)
    crows = rows // CHUNKS
    hrows = crows // 2
    scale = dim ** -0.5

    def remote(src, dst, ss, rs, peer):
        return pltpu.make_async_remote_copy(src_ref=src, dst_ref=dst, send_sem=ss, recv_sem=rs,
                                            device_id={'tp': peer}, device_id_type=pl.DeviceIdType.MESH)

    def other(d):
        return lax.rem(me + d, group)

    def load(src, dst, sem, i):
        part = pl.ds(i * LOAD_ROWS, LOAD_ROWS)
        return pltpu.make_async_copy(src.at[part], dst.at[part], sem.at[i])

    barrier = pltpu.get_barrier_semaphore()
    for d in range(1, group):
        pl.semaphore_signal(barrier, inc=1, device_id={'tp': other(d)}, device_id_type=pl.DeviceIdType.MESH)
    first = [pltpu.make_async_copy(s, d, h_sem.at[i]) for i, (s, d) in enumerate(
        ((hid_h, hid), (wq_h, wq), (lens_h, lens_v), (lens_h.at[0], lens_s)))]
    later = [pltpu.make_async_copy(s, d, h_sem.at[4 + i]) for i, (s, d) in enumerate(
        ((wk_h, wk), (wv_h, wv), (wo_h, wo)))]
    for copy in first + later:
        copy.start()
    first[2].wait()
    first[3].wait()
    pos = jnp.broadcast_to(lens_v[...].astype(F32), (dim // 2, batch)).T
    freq = jnp.exp(lax.broadcasted_iota(jnp.int32, (1, dim // 2), 1).astype(F32) * (-2.0 * math.log(10000.0) / dim))
    angles = pos * freq
    cosr[...] = jnp.cos(angles)
    sinr[...] = jnp.sin(angles)
    first[0].wait()
    first[1].wait()
    for i in range(EARLY):
        load(k_h, k_o, k_sem, i).start()
        load(v_h, v_o, v_sem, i).start()
    q = mm(hid[...], wq[...]).astype(BF16).astype(F32)
    qrot[...] = rope(q, cosr[...], sinr[...]).astype(BF16)
    pl.semaphore_wait(barrier, group - 1)

    qrows = rows // Q_PARTS
    sends = []
    for part in range(Q_PARTS):
        sends.append([])
        for d in range(1, group):
            peer = other(d)
            copy = remote(qrot.at[pl.ds(peer * rows + part * qrows, qrows)], qbuf.at[me, pl.ds(part * qrows, qrows)],
                          q_s.at[part, d], q_r.at[part, d], peer)
            copy.start()
            sends[-1].append(copy)
    qbuf[me] = qrot[own, :]
    for copy in later:
        copy.wait()
    wcopy = remote(wo, wsib, w_s, w_r, chip * 2 + 1 - core)
    wcopy.start()
    mine = hid[own, :]
    k = mm(mine, wk[...]).astype(BF16).astype(F32)
    kn_o[...] = rope(k, cosr[own, :], sinr[own, :]).astype(BF16).astype(F32)
    vn_o[...] = mm(mine, wv[...]).astype(BF16).astype(F32)

    def take_q(part):
        for copy in sends[part]:
            copy.wait()
        for h in range(heads):
            for lane in range(2):
                qf[lane, pl.ds(h * (rows + 1) + part * qrows, qrows), :] = qbuf[
                    h, pl.ds(part * qrows, qrows), lane * LANES:(lane + 1) * LANES].astype(F32)

    take_q(0)
    for i in range(EARLY, rows // LOAD_ROWS):
        load(k_h, k_o, k_sem, i).start()
        load(v_h, v_o, v_sem, i).start()
    slot = lax.broadcasted_iota(jnp.int32, (heads, seq), 1)

    def scores(b):
        n = lens_s[start + b]
        q = jnp.concatenate([qf[lane, pl.ds(b, heads, stride=rows + 1), :] for lane in range(2)], axis=-1)
        s = lax.dot_general(q.astype(BF16), k_o[b], (((1,), (1,)), ((), ())), preferred_element_type=F32) * scale
        s_new = jnp.sum(q * kn_o[pl.ds(b, 1), :], axis=-1, keepdims=True) * scale
        return jnp.where(slot < n, s, -1e30), s_new

    def softmax(s, s_new):
        top = jnp.maximum(jnp.max(s, axis=-1, keepdims=True), s_new)
        e, e_new = jnp.exp(s - top), jnp.exp(s_new - top)
        return e.astype(BF16), e_new.astype(BF16).astype(F32), jnp.sum(e, axis=-1, keepdims=True) + e_new

    def value(b, row, e, e_new, total):
        o = (mm(e, v_o[b]) + e_new * vn_o[pl.ds(b, 1), :]) / total
        return row, o

    def keep(row, o):
        for lane in range(2):
            of[lane, pl.ds(row, heads, stride=crows + 1), :] = o[:, lane * LANES:(lane + 1) * LANES]

    ocopies, ycopies = [], []

    def begin_chunk(ch):
        if ch and (ch * crows) % qrows == 0:
            take_q(ch * crows // qrows)
        for step in range(ch * crows // LOAD_ROWS, (ch + 1) * crows // LOAD_ROWS):
            load(k_h, k_o, k_sem, step).wait()
            load(v_h, v_o, v_sem, step).wait()

    def send_chunk(ch):
        for h in range(heads):
            for half in range(2):
                part = pl.ds(h * (crows + 1) + half * hrows, hrows)
                ob[ch, half, h] = jnp.concatenate([of[lane, part, :] for lane in range(2)], axis=-1).astype(BF16)
        copies = []
        for d in range(1, group):
            peer = other(d)
            pc, ph = lax.div(peer, 2), lax.rem(peer, 2)
            copy = remote(ob.at[ch, ph, pl.ds(pc * 2, 2)], obuf.at[ch, :, me], o_s.at[ch, d], o_r.at[ch, d], peer)
            copy.start()
            copies.append(copy)
        for p in range(2):
            obuf[ch, p, me] = ob[ch, core, chip * 2 + p]
        ocopies.append(copies)

    def project_chunk(ch):
        for copy in ocopies[ch]:
            copy.wait()
        o_own, o_sib = (obuf[ch, p].astype(F32).reshape(heads * hrows, dim).astype(BF16) for p in (core, 1 - core))
        copies = []
        for d in list(range(1, group)) + [0]:
            peer = other(d)
            cols = pl.ds(pl.multiple_of(peer * dim, dim), dim)
            part = (mm(o_own, wo[:, cols]) + mm(o_sib, wsib[:, cols])).astype(BF16)
            if d:
                psend[ch, d] = part
                copy = remote(psend.at[ch, d], ybuf.at[ch, core, chip], y_s.at[ch, d], y_r.at[ch, d], peer)
                copy.start()
                copies.append(copy)
            else:
                ybuf[ch, core, chip] = part
        ycopies.append(copies)

    def sum_chunk(ch):
        for copy in ycopies[ch]:
            copy.wait()
        for h in range(2):
            total = ybuf[ch, h, 0].astype(F32)
            for c in range(1, group // 2):
                total = total + ybuf[ch, h, c].astype(F32)
            for s in range(group):
                yf[pl.ds(s * rows + ch * crows + h * hrows, hrows), :] = total[s * hrows:(s + 1) * hrows]

    per_chunk = crows // GROUP
    ready = None
    for g in range(CHUNKS * per_chunk + 1):
        ch = g // per_chunk
        if ch < CHUNKS and g % per_chunk == 0:
            begin_chunk(ch)
        nxt = [(b, scores(b)) for b in range(g * GROUP, (g + 1) * GROUP)] if ch < CHUNKS else None
        if ready is not None:
            soft = [(b, softmax(*pair)) for b, pair in ready]
            for row, o in [value(b, b % crows, *parts) for b, parts in soft]:
                keep(row, o)
            if g % per_chunk == 0:
                send_chunk(ch - 1)
                if ch == 1:
                    wcopy.wait()
                else:
                    project_chunk(ch - 2)
        ready = nxt
    project_chunk(CHUNKS - 1)
    for ch in range(CHUNKS):
        sum_chunk(ch)
    y_o[...] = yf[...].astype(BF16)


def store_kernel(lens_h, k_i, v_i, kn, vn, y_i, k_o, v_o, y_o, k_v, v_v, lens_s, l_sem, y_sem, k_sem, v_sem, p_sem):
    rows, seq, dim = k_v.shape
    start = lax.axis_index('tp') * rows
    pairs = ((k_v, k_o, k_sem, kn), (v_v, v_o, v_sem, vn))

    def store(pair, i):
        part = pl.ds(i * LOAD_ROWS, LOAD_ROWS)
        return pltpu.make_async_copy(pair[0].at[part], pair[1].at[part], pair[2].at[i])

    lens = pltpu.make_async_copy(lens_h.at[0], lens_s, l_sem)
    lens.start()
    for pair in pairs:
        store(pair, 0).start()
    y_copy = pltpu.make_async_copy(y_i, y_o, y_sem)
    y_copy.start()
    slot = lax.broadcasted_iota(jnp.int32, (PATCH, dim), 0)
    lens.wait()

    def block(b):
        n = lens_s[start + b]
        base = pl.multiple_of(lax.div(n, PATCH) * PATCH, PATCH)
        return n - base, pl.ds(base, PATCH)

    def patch(pair, b):
        at, part = block(b)
        line = jnp.broadcast_to(pair[3][pl.ds(b, 1), :], (PATCH, dim))
        old = pair[0][b, part, :].astype(F32)
        pair[0][b, part, :] = jnp.where(slot == at, line, old).astype(BF16)

    def late(p, b):
        part = block(b)[1]
        return pltpu.make_async_copy(pairs[p][0].at[b, part], pairs[p][1].at[b, part], p_sem.at[p, b])

    def send(i, carry):
        for pair in pairs:
            for r in range(LOAD_ROWS):
                patch(pair, i * LOAD_ROWS + r)
            store(pair, i).start()
        return carry

    lax.fori_loop(1, rows // LOAD_ROWS, send, 0)
    for p in range(2):
        store(pairs[p], 0).wait()
        for b in range(LOAD_ROWS):
            patch(pairs[p], b)
            late(p, b).start()
    for i in range(1, rows // LOAD_ROWS):
        for pair in pairs:
            store(pair, i).wait()
    for p in range(2):
        for b in range(LOAD_ROWS):
            late(p, b).wait()
    y_copy.wait()


def solution(mesh):
    group = mesh.shape['tp']
    cache_spec = P(('dp', 'tp'), None, None)

    def local_step(hidden, w_query, w_key, w_value, w_out, k_cache, v_cache, lengths):
        rows, seq, dim = k_cache.shape
        batch, embed = hidden.shape
        shape = jax.ShapeDtypeStruct
        dma, mib = pltpu.SemaphoreType.DMA, 2 ** 20
        hbm = [pltpu.with_memory_space_constraint(x, pltpu.HBM)
               for x in (lengths.reshape(1, batch), hidden, w_query, w_key, w_value, w_out, k_cache, v_cache)]
        steps = rows // LOAD_ROWS
        crows = rows // CHUNKS
        hrows = crows // 2
        held = pltpu.VMEM(k_cache.shape, BF16)
        k_all, v_all, k_new, v_new, y = pl.pallas_call(
            functools.partial(step_kernel, group),
            out_shape=(held, held, shape((rows, dim), F32), shape((rows, dim), F32), shape((batch, dim), BF16)),
            in_specs=[HBM] * 8,
            out_specs=[VMEM] * 5,
            scratch_shapes=[
                pltpu.SMEM((batch,), jnp.int32), pltpu.VMEM((1, batch), jnp.int32),
                pltpu.VMEM((batch, embed), BF16), pltpu.VMEM((embed, dim), BF16), pltpu.VMEM((embed, dim), BF16),
                pltpu.VMEM((embed, dim), BF16), pltpu.VMEM(w_out.shape, BF16),
                pltpu.VMEM((batch, dim // 2), F32), pltpu.VMEM((batch, dim // 2), F32), pltpu.VMEM((batch, dim), BF16),
                pltpu.VMEM((group, rows, dim), BF16), pltpu.VMEM((2, group * (rows + 1), LANES), F32),
                pltpu.VMEM((2, group * (crows + 1), LANES), F32), pltpu.VMEM((CHUNKS, 2, group, hrows, dim), BF16),
                pltpu.VMEM((CHUNKS, 2, group, hrows, dim), BF16), pltpu.VMEM(w_out.shape, BF16),
                pltpu.VMEM((CHUNKS, group, group * hrows, dim), BF16),
                pltpu.VMEM((CHUNKS, 2, group // 2, group * hrows, dim), BF16), pltpu.VMEM((batch, dim), F32),
                dma((7,)), dma((steps,)), dma((steps,)), dma((Q_PARTS, group)), dma((Q_PARTS, group)), dma, dma,
                dma((CHUNKS, group)), dma((CHUNKS, group)), dma((CHUNKS, group)), dma((CHUNKS, group)),
            ],
            compiler_params=pltpu.CompilerParams(collective_id=0, has_side_effects=True, vmem_limit_bytes=14 * mib),
        )(*hbm)
        k_all, v_all = (pltpu.with_memory_space_constraint(x, pltpu.VMEM) for x in (k_all, v_all))
        k_out, v_out, y, _, _ = pl.pallas_call(
            store_kernel,
            out_shape=(shape(k_cache.shape, BF16), shape(k_cache.shape, BF16), shape((batch, dim), BF16), held, held),
            in_specs=[HBM] + [VMEM] * 5,
            out_specs=[HBM, HBM, HBM, VMEM, VMEM],
            input_output_aliases={1: 3, 2: 4},
            scratch_shapes=[pltpu.SMEM((batch,), jnp.int32), dma, dma, dma((steps,)), dma((steps,)),
                            dma((2, LOAD_ROWS))],
            compiler_params=pltpu.CompilerParams(vmem_limit_bytes=4 * mib),
        )(hbm[0], k_all, v_all, k_new, v_new, y)
        return y, k_out, v_out

    return jax.shard_map(
        local_step,
        mesh=mesh,
        in_specs=(P('dp', None), P(None, 'tp'), P(), P(), P('tp', None), cache_spec, cache_spec, P('dp')),
        out_specs=(P('dp', 'tp'), cache_spec, cache_spec),
        check_vma=False,
    )
```

```python
import functools
import math

import jax
import jax.numpy as jnp
from jax import lax
from jax.experimental import pallas as pl
from jax.experimental.pallas import tpu as pltpu
from jax.sharding import PartitionSpec as P

F32, BF16 = jnp.float32, jnp.bfloat16
HBM = pl.BlockSpec(memory_space=pltpu.HBM)
VMEM = pl.BlockSpec(memory_space=pltpu.VMEM)
LOAD_ROWS = 8
CHUNKS = 4
EARLY = 4
PATCH = 16
LANES = 128
GROUP = 4
Q_PARTS = 2
PEERS = (6, 7, 2, 4, 3, 5, 1)


def mm(a, b):
    return jnp.dot(a, b, preferred_element_type=F32)


def rope(x, cosines, sines):
    half = x.shape[-1] // 2
    x1, x2 = x[:, :half], x[:, half:]
    return jnp.concatenate([x1 * cosines - x2 * sines, x2 * cosines + x1 * sines], axis=-1)


def step_kernel(group, lens_h, hid_h, wq_h, wk_h, wv_h, wo_h, k_h, v_h,
                k_o, v_o, kn_o, vn_o, y_o,
                lens_s, lens_v, hid, wq, wk, wv, wo, cosr, sinr, qrot, qbuf, qf, of, ob, obuf, wsib, psend, ybuf, yf,
                h_sem, k_sem, v_sem, q_s, q_r, w_s, w_r, o_s, o_r, y_s, y_r):
    rows, seq, dim = k_o.shape
    batch = hid.shape[0]
    heads = group
    me = lax.axis_index('tp')
    chip, core = lax.div(me, 2), lax.rem(me, 2)
    start = me * rows
    own = pl.ds(start, rows)
    crows = rows // CHUNKS
    hrows = crows // 2
    scale = dim ** -0.5

    def remote(src, dst, ss, rs, peer):
        return pltpu.make_async_remote_copy(src_ref=src, dst_ref=dst, send_sem=ss, recv_sem=rs,
                                            device_id={'tp': peer}, device_id_type=pl.DeviceIdType.MESH)

    x, y = lax.rem(chip, 2), lax.div(chip, 2)

    def flip(bit, by):
        return 1 - bit if by else bit

    def other(mask):
        return flip(y, mask & 4) * 4 + flip(x, mask & 2) * 2 + flip(core, mask & 1)

    def load(src, dst, sem, i):
        part = pl.ds(i * LOAD_ROWS, LOAD_ROWS)
        return pltpu.make_async_copy(src.at[part], dst.at[part], sem.at[i])

    barrier = pltpu.get_barrier_semaphore()
    for d in PEERS:
        pl.semaphore_signal(barrier, inc=1, device_id={'tp': other(d)}, device_id_type=pl.DeviceIdType.MESH)
    first = [pltpu.make_async_copy(s, d, h_sem.at[i]) for i, (s, d) in enumerate(
        ((hid_h, hid), (wq_h, wq), (lens_h, lens_v), (lens_h.at[0], lens_s)))]
    later = [pltpu.make_async_copy(s, d, h_sem.at[4 + i]) for i, (s, d) in enumerate(
        ((wk_h, wk), (wv_h, wv), (wo_h, wo)))]
    for copy in first + later:
        copy.start()
    first[2].wait()
    first[3].wait()
    pos = jnp.broadcast_to(lens_v[...].astype(F32), (dim // 2, batch)).T
    freq = jnp.exp(lax.broadcasted_iota(jnp.int32, (1, dim // 2), 1).astype(F32) * (-2.0 * math.log(10000.0) / dim))
    angles = pos * freq
    cosr[...] = jnp.cos(angles)
    sinr[...] = jnp.sin(angles)
    first[0].wait()
    first[1].wait()
    for i in range(EARLY):
        load(k_h, k_o, k_sem, i).start()
        load(v_h, v_o, v_sem, i).start()
    q = mm(hid[...], wq[...]).astype(BF16).astype(F32)
    qrot[...] = rope(q, cosr[...], sinr[...]).astype(BF16)
    pl.semaphore_wait(barrier, group - 1)

    qrows = rows // Q_PARTS
    sends = []
    for part in range(Q_PARTS):
        sends.append([])
        for d in PEERS:
            peer = other(d)
            copy = remote(qrot.at[pl.ds(peer * rows + part * qrows, qrows)], qbuf.at[me, pl.ds(part * qrows, qrows)],
                          q_s.at[part, d], q_r.at[part, d], peer)
            copy.start()
            sends[-1].append(copy)
    qbuf[me] = qrot[own, :]
    for copy in later:
        copy.wait()
    wcopy = remote(wo, wsib, w_s, w_r, chip * 2 + 1 - core)
    wcopy.start()
    mine = hid[own, :]
    k = mm(mine, wk[...]).astype(BF16).astype(F32)
    kn_o[...] = rope(k, cosr[own, :], sinr[own, :]).astype(BF16).astype(F32)
    vn_o[...] = mm(mine, wv[...]).astype(BF16).astype(F32)

    def take_q(part):
        for copy in sends[part]:
            copy.wait()
        for h in range(heads):
            for lane in range(2):
                qf[lane, pl.ds(h * (rows + 1) + part * qrows, qrows), :] = qbuf[
                    h, pl.ds(part * qrows, qrows), lane * LANES:(lane + 1) * LANES].astype(F32)

    take_q(0)
    for i in range(EARLY, rows // LOAD_ROWS):
        load(k_h, k_o, k_sem, i).start()
        load(v_h, v_o, v_sem, i).start()
    slot = lax.broadcasted_iota(jnp.int32, (heads, seq), 1)

    def scores(b):
        n = lens_s[start + b]
        q = jnp.concatenate([qf[lane, pl.ds(b, heads, stride=rows + 1), :] for lane in range(2)], axis=-1)
        s = lax.dot_general(q.astype(BF16), k_o[b], (((1,), (1,)), ((), ())), preferred_element_type=F32) * scale
        s_new = jnp.sum(q * kn_o[pl.ds(b, 1), :], axis=-1, keepdims=True) * scale
        return jnp.where(slot < n, s, -1e30), s_new

    def softmax(s, s_new):
        top = jnp.maximum(jnp.max(s, axis=-1, keepdims=True), s_new)
        e, e_new = jnp.exp(s - top), jnp.exp(s_new - top)
        return e.astype(BF16), e_new.astype(BF16).astype(F32), jnp.sum(e, axis=-1, keepdims=True) + e_new

    def attend(first_row, crow):
        groups = [range(g, g + GROUP) for g in range(0, crow, GROUP)]
        ready = None
        for g in range(len(groups) + 1):
            nxt = [scores(first_row + u) for u in groups[g]] if g < len(groups) else None
            if ready is not None:
                soft = [softmax(*pair) for pair in ready]
                outs = [mm(e, v_o[first_row + u]) for (e, _, _), u in zip(soft, groups[g - 1])]
                for o, (_, e_new, total), u in zip(outs, soft, groups[g - 1]):
                    o = (o + e_new * vn_o[pl.ds(first_row + u, 1), :]) / total
                    for lane in range(2):
                        of[lane, pl.ds(u, heads, stride=crow + 1), :] = o[:, lane * LANES:(lane + 1) * LANES]
            ready = nxt

    ocopies, ycopies = [], []

    def attend_chunk(ch):
        for step in range(ch * crows // LOAD_ROWS, (ch + 1) * crows // LOAD_ROWS):
            load(k_h, k_o, k_sem, step).wait()
            load(v_h, v_o, v_sem, step).wait()
        attend(ch * crows, crows)
        for h in range(heads):
            for half in range(2):
                part = pl.ds(h * (crows + 1) + half * hrows, hrows)
                ob[ch, half, h] = jnp.concatenate([of[lane, part, :] for lane in range(2)], axis=-1).astype(BF16)
        copies = []
        for d in PEERS:
            peer = other(d)
            pc, ph = lax.div(peer, 2), lax.rem(peer, 2)
            copy = remote(ob.at[ch, ph, pl.ds(pc * 2, 2)], obuf.at[ch, :, me], o_s.at[ch, d], o_r.at[ch, d], peer)
            copy.start()
            copies.append(copy)
        for p in range(2):
            obuf[ch, p, me] = ob[ch, core, chip * 2 + p]
        ocopies.append(copies)

    def project_chunk(ch):
        for copy in ocopies[ch]:
            copy.wait()
        o_own, o_sib = (obuf[ch, p].astype(F32).reshape(heads * hrows, dim).astype(BF16) for p in (core, 1 - core))
        copies = []
        for d in PEERS + (0,):
            peer = other(d)
            cols = pl.ds(pl.multiple_of(peer * dim, dim), dim)
            part = (mm(o_own, wo[:, cols]) + mm(o_sib, wsib[:, cols])).astype(BF16)
            if d:
                psend[ch, d] = part
                copy = remote(psend.at[ch, d], ybuf.at[ch, core, chip], y_s.at[ch, d], y_r.at[ch, d], peer)
                copy.start()
                copies.append(copy)
            else:
                ybuf[ch, core, chip] = part
        ycopies.append(copies)

    def sum_chunk(ch):
        for copy in ycopies[ch]:
            copy.wait()
        for h in range(2):
            total = ybuf[ch, h, 0].astype(F32)
            for c in range(1, group // 2):
                total = total + ybuf[ch, h, c].astype(F32)
            for s in range(group):
                yf[pl.ds(s * rows + ch * crows + h * hrows, hrows), :] = total[s * hrows:(s + 1) * hrows]

    for ch in range(CHUNKS):
        if ch and (ch * crows) % qrows == 0:
            take_q(ch * crows // qrows)
        attend_chunk(ch)
        if ch == 0:
            wcopy.wait()
        else:
            project_chunk(ch - 1)
    project_chunk(CHUNKS - 1)
    for ch in range(CHUNKS):
        sum_chunk(ch)
    y_o[...] = yf[...].astype(BF16)


def store_kernel(lens_h, k_i, v_i, kn, vn, y_i, k_o, v_o, y_o, k_v, v_v, lens_s, l_sem, y_sem, k_sem, v_sem, p_sem):
    rows, seq, dim = k_v.shape
    start = lax.axis_index('tp') * rows
    pairs = ((k_v, k_o, k_sem, kn), (v_v, v_o, v_sem, vn))

    def store(pair, i):
        part = pl.ds(i * LOAD_ROWS, LOAD_ROWS)
        return pltpu.make_async_copy(pair[0].at[part], pair[1].at[part], pair[2].at[i])

    lens = pltpu.make_async_copy(lens_h.at[0], lens_s, l_sem)
    lens.start()
    for pair in pairs:
        store(pair, 0).start()
    y_copy = pltpu.make_async_copy(y_i, y_o, y_sem)
    y_copy.start()
    slot = lax.broadcasted_iota(jnp.int32, (PATCH, dim), 0)
    lens.wait()

    def block(b):
        n = lens_s[start + b]
        base = pl.multiple_of(lax.div(n, PATCH) * PATCH, PATCH)
        return n - base, pl.ds(base, PATCH)

    def patch(pair, b):
        at, part = block(b)
        line = jnp.broadcast_to(pair[3][pl.ds(b, 1), :], (PATCH, dim))
        old = pair[0][b, part, :].astype(F32)
        pair[0][b, part, :] = jnp.where(slot == at, line, old).astype(BF16)

    def late(p, b):
        part = block(b)[1]
        return pltpu.make_async_copy(pairs[p][0].at[b, part], pairs[p][1].at[b, part], p_sem.at[p, b])

    def send(i, carry):
        for pair in pairs:
            for r in range(LOAD_ROWS):
                patch(pair, i * LOAD_ROWS + r)
            store(pair, i).start()
        return carry

    lax.fori_loop(1, rows // LOAD_ROWS, send, 0)
    for p in range(2):
        store(pairs[p], 0).wait()
        for b in range(LOAD_ROWS):
            patch(pairs[p], b)
            late(p, b).start()
    for i in range(1, rows // LOAD_ROWS):
        for pair in pairs:
            store(pair, i).wait()
    for p in range(2):
        for b in range(LOAD_ROWS):
            late(p, b).wait()
    y_copy.wait()


def solution(mesh):
    group = mesh.shape['tp']
    cache_spec = P(('dp', 'tp'), None, None)

    def local_step(hidden, w_query, w_key, w_value, w_out, k_cache, v_cache, lengths):
        rows, seq, dim = k_cache.shape
        batch, embed = hidden.shape
        shape = jax.ShapeDtypeStruct
        dma, mib = pltpu.SemaphoreType.DMA, 2 ** 20
        hbm = [pltpu.with_memory_space_constraint(x, pltpu.HBM)
               for x in (lengths.reshape(1, batch), hidden, w_query, w_key, w_value, w_out, k_cache, v_cache)]
        steps = rows // LOAD_ROWS
        crows = rows // CHUNKS
        hrows = crows // 2
        held = pltpu.VMEM(k_cache.shape, BF16)
        k_all, v_all, k_new, v_new, y = pl.pallas_call(
            functools.partial(step_kernel, group),
            out_shape=(held, held, shape((rows, dim), F32), shape((rows, dim), F32), shape((batch, dim), BF16)),
            in_specs=[HBM] * 8,
            out_specs=[VMEM] * 5,
            scratch_shapes=[
                pltpu.SMEM((batch,), jnp.int32), pltpu.VMEM((1, batch), jnp.int32),
                pltpu.VMEM((batch, embed), BF16), pltpu.VMEM((embed, dim), BF16), pltpu.VMEM((embed, dim), BF16),
                pltpu.VMEM((embed, dim), BF16), pltpu.VMEM(w_out.shape, BF16),
                pltpu.VMEM((batch, dim // 2), F32), pltpu.VMEM((batch, dim // 2), F32), pltpu.VMEM((batch, dim), BF16),
                pltpu.VMEM((group, rows, dim), BF16), pltpu.VMEM((2, group * (rows + 1), LANES), F32),
                pltpu.VMEM((2, group * (crows + 1), LANES), F32), pltpu.VMEM((CHUNKS, 2, group, hrows, dim), BF16),
                pltpu.VMEM((CHUNKS, 2, group, hrows, dim), BF16), pltpu.VMEM(w_out.shape, BF16),
                pltpu.VMEM((CHUNKS, group, group * hrows, dim), BF16),
                pltpu.VMEM((CHUNKS, 2, group // 2, group * hrows, dim), BF16), pltpu.VMEM((batch, dim), F32),
                dma((7,)), dma((steps,)), dma((steps,)), dma((Q_PARTS, group)), dma((Q_PARTS, group)), dma, dma,
                dma((CHUNKS, group)), dma((CHUNKS, group)), dma((CHUNKS, group)), dma((CHUNKS, group)),
            ],
            compiler_params=pltpu.CompilerParams(collective_id=0, has_side_effects=True, vmem_limit_bytes=14 * mib),
        )(*hbm)
        k_all, v_all = (pltpu.with_memory_space_constraint(x, pltpu.VMEM) for x in (k_all, v_all))
        k_out, v_out, y, _, _ = pl.pallas_call(
            store_kernel,
            out_shape=(shape(k_cache.shape, BF16), shape(k_cache.shape, BF16), shape((batch, dim), BF16), held, held),
            in_specs=[HBM] + [VMEM] * 5,
            out_specs=[HBM, HBM, HBM, VMEM, VMEM],
            input_output_aliases={1: 3, 2: 4},
            scratch_shapes=[pltpu.SMEM((batch,), jnp.int32), dma, dma, dma((steps,)), dma((steps,)),
                            dma((2, LOAD_ROWS))],
            compiler_params=pltpu.CompilerParams(vmem_limit_bytes=4 * mib),
        )(hbm[0], k_all, v_all, k_new, v_new, y)
        return y, k_out, v_out

    return jax.shard_map(
        local_step,
        mesh=mesh,
        in_specs=(P('dp', None), P(None, 'tp'), P(), P(), P('tp', None), cache_spec, cache_spec, P('dp')),
        out_specs=(P('dp', 'tp'), cache_spec, cache_spec),
        check_vma=False,
    )
```

```python
import functools
import math

import jax
import jax.numpy as jnp
from jax import lax
from jax.experimental import pallas as pl
from jax.experimental.pallas import tpu as pltpu
from jax.sharding import PartitionSpec as P

F32, BF16 = jnp.float32, jnp.bfloat16
HBM = pl.BlockSpec(memory_space=pltpu.HBM)
VMEM = pl.BlockSpec(memory_space=pltpu.VMEM)
LOAD_ROWS = 8
CHUNKS = 4
PATCH = 16
LANES = 128
GROUP = 4
Q_PARTS = 4
PEERS = (6, 7, 2, 4, 3, 5, 1)


def mm(a, b):
    return jnp.dot(a, b, preferred_element_type=F32)


def rope(x, cosines, sines):
    half = x.shape[-1] // 2
    x1, x2 = x[:, :half], x[:, half:]
    return jnp.concatenate([x1 * cosines - x2 * sines, x2 * cosines + x1 * sines], axis=-1)


def step_kernel(group, lens_h, hid_h, wq_h, wk_h, wv_h, wo_h, k_h, v_h,
                k_o, v_o, kn_o, vn_o, y_o,
                lens_s, lens_v, hid, wq, wk, wv, wo, cosr, sinr, qrot, qbuf, qf, of, ob, obuf, wsib, psend, ybuf, yf,
                h_sem, k_sem, v_sem, q_s, q_r, w_s, w_r, o_s, o_r, y_s, y_r):
    rows, seq, dim = k_o.shape
    batch = hid.shape[0]
    heads = group
    me = lax.axis_index('tp')
    chip, core = lax.div(me, 2), lax.rem(me, 2)
    start = me * rows
    own = pl.ds(start, rows)
    crows = rows // CHUNKS
    hrows = crows // 2
    scale = dim ** -0.5

    def remote(src, dst, ss, rs, peer):
        return pltpu.make_async_remote_copy(src_ref=src, dst_ref=dst, send_sem=ss, recv_sem=rs,
                                            device_id={'tp': peer}, device_id_type=pl.DeviceIdType.MESH)

    x, y = lax.rem(chip, 2), lax.div(chip, 2)

    def flip(bit, by):
        return 1 - bit if by else bit

    def other(mask):
        return flip(y, mask & 4) * 4 + flip(x, mask & 2) * 2 + flip(core, mask & 1)

    def load(src, dst, sem, i):
        part = pl.ds(i * LOAD_ROWS, LOAD_ROWS)
        return pltpu.make_async_copy(src.at[part], dst.at[part], sem.at[i])

    def wave(ch):
        for i in range(ch * crows // LOAD_ROWS, (ch + 1) * crows // LOAD_ROWS):
            load(k_h, k_o, k_sem, i).start()
            load(v_h, v_o, v_sem, i).start()

    barrier = pltpu.get_barrier_semaphore()
    for d in PEERS:
        pl.semaphore_signal(barrier, inc=1, device_id={'tp': other(d)}, device_id_type=pl.DeviceIdType.MESH)
    first = [pltpu.make_async_copy(s, d, h_sem.at[i]) for i, (s, d) in enumerate(
        ((hid_h, hid), (wq_h, wq), (lens_h, lens_v), (lens_h.at[0], lens_s)))]
    later = [pltpu.make_async_copy(s, d, h_sem.at[4 + i]) for i, (s, d) in enumerate(
        ((wk_h, wk), (wv_h, wv), (wo_h, wo)))]
    for copy in first + later:
        copy.start()
    first[2].wait()
    first[3].wait()
    pos = jnp.broadcast_to(lens_v[...].astype(F32), (dim // 2, batch)).T
    freq = jnp.exp(lax.broadcasted_iota(jnp.int32, (1, dim // 2), 1).astype(F32) * (-2.0 * math.log(10000.0) / dim))
    angles = pos * freq
    cosr[...] = jnp.cos(angles)
    sinr[...] = jnp.sin(angles)
    first[0].wait()
    first[1].wait()
    wave(0)
    q = mm(hid[...], wq[...]).astype(BF16).astype(F32)
    qrot[...] = rope(q, cosr[...], sinr[...]).astype(BF16)
    pl.semaphore_wait(barrier, group - 1)

    qrows = rows // Q_PARTS
    sends = []
    for part in range(Q_PARTS):
        sends.append([])
        for d in PEERS:
            peer = other(d)
            copy = remote(qrot.at[pl.ds(peer * rows + part * qrows, qrows)], qbuf.at[me, pl.ds(part * qrows, qrows)],
                          q_s.at[part, d], q_r.at[part, d], peer)
            copy.start()
            sends[-1].append(copy)
    qbuf[me] = qrot[own, :]
    for copy in later:
        copy.wait()
    wave(1)
    wcopy = remote(wo, wsib, w_s, w_r, chip * 2 + 1 - core)
    wcopy.start()
    mine = hid[own, :]
    k = mm(mine, wk[...]).astype(BF16).astype(F32)
    kn_o[...] = rope(k, cosr[own, :], sinr[own, :]).astype(BF16).astype(F32)
    vn_o[...] = mm(mine, wv[...]).astype(BF16).astype(F32)

    def take_q(part):
        for copy in sends[part]:
            copy.wait()
        for h in range(heads):
            for lane in range(2):
                qf[lane, pl.ds(h * (rows + 1) + part * qrows, qrows), :] = qbuf[
                    h, pl.ds(part * qrows, qrows), lane * LANES:(lane + 1) * LANES].astype(F32)

    take_q(0)
    wave(2)
    slot = lax.broadcasted_iota(jnp.int32, (heads, seq), 1)

    def scores(b):
        n = lens_s[start + b]
        q = jnp.concatenate([qf[lane, pl.ds(b, heads, stride=rows + 1), :] for lane in range(2)], axis=-1)
        s = lax.dot_general(q.astype(BF16), k_o[b], (((1,), (1,)), ((), ())), preferred_element_type=F32) * scale
        s_new = jnp.sum(q * kn_o[pl.ds(b, 1), :], axis=-1, keepdims=True) * scale
        return jnp.where(slot < n, s, -1e30), s_new

    def softmax(s, s_new):
        top = jnp.maximum(jnp.max(s, axis=-1, keepdims=True), s_new)
        e, e_new = jnp.exp(s - top), jnp.exp(s_new - top)
        return e.astype(BF16), e_new.astype(BF16).astype(F32), jnp.sum(e, axis=-1, keepdims=True) + e_new

    def attend(first_row, crow):
        groups = [range(g, g + GROUP) for g in range(0, crow, GROUP)]
        ready = None
        for g in range(len(groups) + 1):
            nxt = [scores(first_row + u) for u in groups[g]] if g < len(groups) else None
            if ready is not None:
                soft = [softmax(*pair) for pair in ready]
                outs = [mm(e, v_o[first_row + u]) for (e, _, _), u in zip(soft, groups[g - 1])]
                for o, (_, e_new, total), u in zip(outs, soft, groups[g - 1]):
                    o = (o + e_new * vn_o[pl.ds(first_row + u, 1), :]) / total
                    for lane in range(2):
                        of[lane, pl.ds(u, heads, stride=crow + 1), :] = o[:, lane * LANES:(lane + 1) * LANES]
            ready = nxt

    ocopies, ycopies = [], []

    def attend_chunk(ch):
        for step in range(ch * crows // LOAD_ROWS, (ch + 1) * crows // LOAD_ROWS):
            load(k_h, k_o, k_sem, step).wait()
            load(v_h, v_o, v_sem, step).wait()
        attend(ch * crows, crows)
        for h in range(heads):
            for half in range(2):
                part = pl.ds(h * (crows + 1) + half * hrows, hrows)
                ob[ch, half, h] = jnp.concatenate([of[lane, part, :] for lane in range(2)], axis=-1).astype(BF16)
        copies = []
        for d in PEERS:
            peer = other(d)
            pc, ph = lax.div(peer, 2), lax.rem(peer, 2)
            copy = remote(ob.at[ch, ph, pl.ds(pc * 2, 2)], obuf.at[ch, :, me], o_s.at[ch, d], o_r.at[ch, d], peer)
            copy.start()
            copies.append(copy)
        for p in range(2):
            obuf[ch, p, me] = ob[ch, core, chip * 2 + p]
        ocopies.append(copies)

    def project_chunk(ch):
        for copy in ocopies[ch]:
            copy.wait()
        o_own, o_sib = (obuf[ch, p].astype(F32).reshape(heads * hrows, dim).astype(BF16) for p in (core, 1 - core))
        copies = []
        for d in PEERS + (0,):
            peer = other(d)
            cols = pl.ds(pl.multiple_of(peer * dim, dim), dim)
            part = (mm(o_own, wo[:, cols]) + mm(o_sib, wsib[:, cols])).astype(BF16)
            if d:
                psend[ch, d] = part
                copy = remote(psend.at[ch, d], ybuf.at[ch, core, chip], y_s.at[ch, d], y_r.at[ch, d], peer)
                copy.start()
                copies.append(copy)
            else:
                ybuf[ch, core, chip] = part
        ycopies.append(copies)

    def sum_chunk(ch):
        for copy in ycopies[ch]:
            copy.wait()
        for h in range(2):
            total = ybuf[ch, h, 0].astype(F32)
            for c in range(1, group // 2):
                total = total + ybuf[ch, h, c].astype(F32)
            for s in range(group):
                yf[pl.ds(s * rows + ch * crows + h * hrows, hrows), :] = total[s * hrows:(s + 1) * hrows]

    for ch in range(CHUNKS):
        if ch and (ch * crows) % qrows == 0:
            take_q(ch * crows // qrows)
        attend_chunk(ch)
        if ch + 3 < CHUNKS:
            wave(ch + 3)
        if ch == 0:
            wcopy.wait()
        else:
            project_chunk(ch - 1)
    project_chunk(CHUNKS - 1)
    for ch in range(CHUNKS):
        sum_chunk(ch)
    y_o[...] = yf[...].astype(BF16)


def store_kernel(lens_h, k_i, v_i, kn, vn, y_i, k_o, v_o, y_o, k_v, v_v, lens_s, l_sem, y_sem, k_sem, v_sem, p_sem):
    rows, seq, dim = k_v.shape
    start = lax.axis_index('tp') * rows
    pairs = ((k_v, k_o, k_sem, kn), (v_v, v_o, v_sem, vn))

    def store(pair, i):
        part = pl.ds(i * LOAD_ROWS, LOAD_ROWS)
        return pltpu.make_async_copy(pair[0].at[part], pair[1].at[part], pair[2].at[i])

    lens = pltpu.make_async_copy(lens_h.at[0], lens_s, l_sem)
    lens.start()
    for pair in pairs:
        store(pair, 0).start()
    y_copy = pltpu.make_async_copy(y_i, y_o, y_sem)
    y_copy.start()
    slot = lax.broadcasted_iota(jnp.int32, (PATCH, dim), 0)
    lens.wait()

    def block(b):
        n = lens_s[start + b]
        base = pl.multiple_of(lax.div(n, PATCH) * PATCH, PATCH)
        return n - base, pl.ds(base, PATCH)

    def patch(pair, b):
        at, part = block(b)
        line = jnp.broadcast_to(pair[3][pl.ds(b, 1), :], (PATCH, dim))
        old = pair[0][b, part, :].astype(F32)
        pair[0][b, part, :] = jnp.where(slot == at, line, old).astype(BF16)

    def late(p, b):
        part = block(b)[1]
        return pltpu.make_async_copy(pairs[p][0].at[b, part], pairs[p][1].at[b, part], p_sem.at[p, b])

    def send(i, carry):
        for pair in pairs:
            for r in range(LOAD_ROWS):
                patch(pair, i * LOAD_ROWS + r)
            store(pair, i).start()
        return carry

    lax.fori_loop(1, rows // LOAD_ROWS, send, 0)
    for p in range(2):
        store(pairs[p], 0).wait()
        for b in range(LOAD_ROWS):
            patch(pairs[p], b)
            late(p, b).start()
    for i in range(1, rows // LOAD_ROWS):
        for pair in pairs:
            store(pair, i).wait()
    for p in range(2):
        for b in range(LOAD_ROWS):
            late(p, b).wait()
    y_copy.wait()


def solution(mesh):
    group = mesh.shape['tp']
    cache_spec = P(('dp', 'tp'), None, None)

    def local_step(hidden, w_query, w_key, w_value, w_out, k_cache, v_cache, lengths):
        rows, seq, dim = k_cache.shape
        batch, embed = hidden.shape
        shape = jax.ShapeDtypeStruct
        dma, mib = pltpu.SemaphoreType.DMA, 2 ** 20
        hbm = [pltpu.with_memory_space_constraint(x, pltpu.HBM)
               for x in (lengths.reshape(1, batch), hidden, w_query, w_key, w_value, w_out, k_cache, v_cache)]
        steps = rows // LOAD_ROWS
        crows = rows // CHUNKS
        hrows = crows // 2
        held = pltpu.VMEM(k_cache.shape, BF16)
        k_all, v_all, k_new, v_new, y = pl.pallas_call(
            functools.partial(step_kernel, group),
            out_shape=(held, held, shape((rows, dim), F32), shape((rows, dim), F32), shape((batch, dim), BF16)),
            in_specs=[HBM] * 8,
            out_specs=[VMEM] * 5,
            scratch_shapes=[
                pltpu.SMEM((batch,), jnp.int32), pltpu.VMEM((1, batch), jnp.int32),
                pltpu.VMEM((batch, embed), BF16), pltpu.VMEM((embed, dim), BF16), pltpu.VMEM((embed, dim), BF16),
                pltpu.VMEM((embed, dim), BF16), pltpu.VMEM(w_out.shape, BF16),
                pltpu.VMEM((batch, dim // 2), F32), pltpu.VMEM((batch, dim // 2), F32), pltpu.VMEM((batch, dim), BF16),
                pltpu.VMEM((group, rows, dim), BF16), pltpu.VMEM((2, group * (rows + 1), LANES), F32),
                pltpu.VMEM((2, group * (crows + 1), LANES), F32), pltpu.VMEM((CHUNKS, 2, group, hrows, dim), BF16),
                pltpu.VMEM((CHUNKS, 2, group, hrows, dim), BF16), pltpu.VMEM(w_out.shape, BF16),
                pltpu.VMEM((CHUNKS, group, group * hrows, dim), BF16),
                pltpu.VMEM((CHUNKS, 2, group // 2, group * hrows, dim), BF16), pltpu.VMEM((batch, dim), F32),
                dma((7,)), dma((steps,)), dma((steps,)), dma((Q_PARTS, group)), dma((Q_PARTS, group)), dma, dma,
                dma((CHUNKS, group)), dma((CHUNKS, group)), dma((CHUNKS, group)), dma((CHUNKS, group)),
            ],
            compiler_params=pltpu.CompilerParams(collective_id=0, has_side_effects=True, vmem_limit_bytes=14 * mib),
        )(*hbm)
        k_all, v_all = (pltpu.with_memory_space_constraint(x, pltpu.VMEM) for x in (k_all, v_all))
        k_out, v_out, y, _, _ = pl.pallas_call(
            store_kernel,
            out_shape=(shape(k_cache.shape, BF16), shape(k_cache.shape, BF16), shape((batch, dim), BF16), held, held),
            in_specs=[HBM] + [VMEM] * 5,
            out_specs=[HBM, HBM, HBM, VMEM, VMEM],
            input_output_aliases={1: 3, 2: 4},
            scratch_shapes=[pltpu.SMEM((batch,), jnp.int32), dma, dma, dma((steps,)), dma((steps,)),
                            dma((2, LOAD_ROWS))],
            compiler_params=pltpu.CompilerParams(vmem_limit_bytes=4 * mib),
        )(hbm[0], k_all, v_all, k_new, v_new, y)
        return y, k_out, v_out

    return jax.shard_map(
        local_step,
        mesh=mesh,
        in_specs=(P('dp', None), P(None, 'tp'), P(), P(), P('tp', None), cache_spec, cache_spec, P('dp')),
        out_specs=(P('dp', 'tp'), cache_spec, cache_spec),
        check_vma=False,
    )
```
